8 devices in a mesh: dp: 1 (over z), tp: 8 (over x, y, core).
Axes of the slice: x: 2, y: 2, z: 1, core: 2. Of those that a mesh axis runs over, the one named last changes fastest.
Arguments:
- x: bfloat16 [2048, 7168], P(('dp', 'tp'))
- dy: bfloat16 [2048, 7168], P(('dp', 'tp'))
- gain: bfloat16 [7168], replicated
- wq: bfloat16 [7168, 7168], P(None, 'tp')
- wk: bfloat16 [7168, 1024], P(None, 'tp')
- wv: bfloat16 [7168, 1024], P(None, 'tp')
- wo: bfloat16 [7168, 7168], P('tp')
Outputs:
- output 1: bfloat16 [2048, 7168], P(('dp', 'tp'))
- output 2: float32 [1, 7168], P('dp')
- output 3: bfloat16 [7168, 7168], P('dp', 'tp')
- output 4: bfloat16 [7168, 1024], P('dp', 'tp')
- output 5: bfloat16 [7168, 1024], P('dp', 'tp')
- output 6: bfloat16 [7168, 7168], P(('dp', 'tp'))
All inputs are finite; a program needn't handle non-finite values.
Results may differ from the reference program's by a relative error of at most 0.018.
Values are sent between devices in bfloat16 or wider.
A program may use at most 2 GiB of HBM per device.

```python
import jax
import jax.numpy as jnp
from jax import lax

ROWS = 2048
D = 7168
HEADS = 56
KV_HEADS = 8
HEAD = 128
THETA = 10000


def setup_inputs(seed: int = 0, part: int = 0) -> dict:
    kx, ky, kn, kq, kk, kv, ko = jax.random.split(jax.random.key(seed), 7)

    def weights(key, rows, columns):
        return jax.random.normal(key, (rows, columns), jnp.float32) * rows**-0.5

    drawn = {
        "x": jax.random.normal(jax.random.fold_in(kx, part), (ROWS, D), jnp.float32),
        "dy": jax.random.normal(jax.random.fold_in(ky, part), (ROWS, D), jnp.float32) * ROWS**-0.5,
        "gain": 1 + 0.1 * jax.random.normal(kn, (D,), jnp.float32),
        "wq": 2 * weights(kq, D, HEADS * HEAD),
        "wk": 2 * weights(kk, D, KV_HEADS * HEAD),
        "wv": 4 * weights(kv, D, KV_HEADS * HEAD),
        "wo": weights(ko, HEADS * HEAD, D),
    }
    return {k: v.astype(jnp.bfloat16) for k, v in drawn.items()}


def normed(x, gain):
    wide = x.astype(jnp.float32)
    scale = lax.rsqrt(jnp.mean(wide * wide, -1, keepdims=True) + 1e-6)
    return (wide * scale * gain.astype(jnp.float32)).astype(jnp.bfloat16)


def turned(t, place, theta):
    half = t.shape[-1] // 2
    angle = place.astype(jnp.float32)[:, None] * theta ** (-jnp.arange(half, dtype=jnp.float32) / half)
    cos, sin = jnp.cos(angle)[:, None], jnp.sin(angle)[:, None]
    a, b = t[..., :half].astype(jnp.float32), t[..., half:].astype(jnp.float32)
    return jnp.concatenate([a * cos - b * sin, b * cos + a * sin], -1).astype(jnp.bfloat16)


def matmul(a, w):
    return jnp.dot(a, w, preferred_element_type=jnp.float32).astype(jnp.bfloat16)


def einsum(form, a, b):
    return jnp.einsum(form, a.astype(jnp.float32), b.astype(jnp.float32))


def attention(q, k, v):
    scores = einsum("tgsd,ugd->gstu", q, k) * q.shape[-1] ** -0.5
    token = jnp.arange(q.shape[0])
    scores = jnp.where(token[:, None] >= token, scores, -jnp.inf)
    weights = jax.nn.softmax(scores, -1).astype(jnp.bfloat16)
    return einsum("gstu,ugd->tgsd", weights, v).astype(jnp.bfloat16)


def forward(x, gain, wq, wk, wv, wo):
    rows = x.shape[0]
    a, place = normed(x, gain), jnp.arange(rows)
    k = turned(matmul(a, wk).reshape(rows, -1, HEAD), place, THETA)
    q = turned(matmul(a, wq).reshape(rows, -1, HEAD), place, THETA).reshape(rows, k.shape[1], -1, HEAD)
    v = matmul(a, wv).reshape(rows, -1, HEAD)
    seen = attention(q, k, v).reshape(rows, -1)
    return (x.astype(jnp.float32) + jnp.dot(seen, wo, preferred_element_type=jnp.float32)).astype(jnp.bfloat16)


def reference(x, dy, gain, wq, wk, wv, wo):
    _, back = jax.vjp(forward, x, gain.astype(jnp.float32), wq, wk, wv, wo)
    by_x, by_gain, *by_weights = back(dy)
    return (by_x, by_gain[None], *by_weights)
```

```python
import functools

import jax
import jax.numpy as jnp
from jax import lax
from jax.experimental import pallas as pl
from jax.experimental.pallas import tpu as pltpu
from jax.sharding import PartitionSpec as P


HEAD = 128
THETA = 10000
NEG = -1e30
HIDDEN = 2 * NEG
LOG2E = 1.4426950408889634
VMEM = 60 * 2**20
F32, BF16 = jnp.float32, jnp.bfloat16
ANY = pl.BlockSpec(memory_space=pl.ANY)
TOKEN = jax.ShapeDtypeStruct((8, 128), F32)
TOKEN_SPEC = pl.BlockSpec(TOKEN.shape, lambda i, _: (0, 0))


def _dot(a, b, ca, cb):
    return lax.dot_general(a, b, (((ca,), (cb,)), ((), ())), preferred_element_type=F32)


def _params():
    return pltpu.CompilerParams(dimension_semantics=("arbitrary",), vmem_limit_bytes=VMEM)


def _cost(products):
    return pl.CostEstimate(flops=2 * products, bytes_accessed=products // 64, transcendentals=0)


def _whole(*shape):
    return pl.BlockSpec(shape, lambda i, _: (0, 0))


HALF = 128


def _at(me, key):
    return pl.multiple_of(((me[0] ^ key[0]) * 2 + key[1]) * HALF, HALF)


def _rows(n):
    return [pl.ds(i * HALF, HALF) for i in range(n)]


def _parts(size):
    step = size // 7
    return [pl.ds(lo * step, (hi - lo) * step) for lo, hi in ((0, 1), (1, 3), (3, 5), (5, 7))]


class _Copies:
    def __init__(self, sem):
        self.sem, self.used = sem, 0

    def start(self, pairs):
        made = []
        for src, dst in pairs:
            made.append(pltpu.make_async_copy(src, dst, self.sem.at[self.used]))
            made[-1].start()
            self.used += 1
        return made


def _wait(copies):
    for c in copies:
        c.wait()


def _stacked(weights, w_s, part):
    at, pairs = 0, []
    for w in weights:
        pairs.append((w.at[part, :], w_s.at[part, at : at + w.shape[1]]))
        at += w.shape[1]
    return pairs


def _project(me, dep, *refs, keys, heads, extra, through):
    n = len(keys)
    pieces, (wq, wk, wv, cos, sin), refs = refs[:n], refs[n : n + 5], refs[n + 5 + extra :]
    q_hbm, k_hbm, v_hbm, a_hbm = refs[:4]
    tok, a_s, w_s, cos_s, sin_s, acc, q_s, k_s, v_s, sem = refs[4 + through :]
    tok[...] = jnp.zeros_like(tok)
    rows, tokens = _rows(n), [pl.ds(_at(me, key), HALF) for key in keys]
    copies, parts = _Copies(sem), _parts(a_s.shape[1])
    loads = [copies.start([(p.at[:, part], a_s.at[r, part]) for p, r in zip(pieces, rows)] + _stacked((wq, wk, wv), w_s, part)) for part in parts]
    loads[-1] += copies.start([(t.at[there, :], s.at[r, :]) for t, s in ((cos, cos_s), (sin, sin_s)) for r, there in zip(rows, tokens)])
    for c, part in enumerate(parts):
        _wait(loads[c])
        if part is parts[-1]:
            stores = copies.start([(a_s.at[r, :], a_hbm.at[there, :]) for r, there in zip(rows, tokens)])
        got = _dot(a_s[:, part], w_s[part, :], 1, 0)
        acc[...] = got if c == 0 else acc[...] + got
    for h in range(heads + 2):
        t = acc[:, h * HEAD : (h + 1) * HEAD].astype(BF16)
        if h <= heads:
            t = t.astype(F32)
            t = (t * cos_s[...] + pltpu.roll(t, HEAD // 2, 1) * sin_s[...]).astype(BF16)
        if h < heads:
            q_s[h] = t
        else:
            (k_s if h == heads else v_s)[...] = t
    for r, there in zip(rows, tokens):
        stores += copies.start([(q_s.at[:, r, :], q_hbm.at[:, there, :]), (k_s.at[r, :], k_hbm.at[there, :]), (v_s.at[r, :], v_hbm.at[there, :])])
    _wait(stores)


def project(dep, me, pieces, keys, weights, cos, sin, before, through=()):
    (d, width), more = weights[0].shape, weights[1].shape[1]
    heads, rows, n, full = width // HEAD, cos.shape[0], len(pieces), width + 2 * more
    total, extra = n * HALF, len(before) + len(through)
    outs = [jax.ShapeDtypeStruct(s, BF16) for s in ((heads, rows, HEAD), (rows, HEAD), (rows, HEAD), (rows, d))]
    outs += [jax.ShapeDtypeStruct(t.shape, t.dtype) for t in through]
    first = 2 + n + 5
    return pl.pallas_call(
        functools.partial(_project, keys=keys, heads=heads, extra=extra, through=len(through)),
        grid_spec=pltpu.PrefetchScalarGridSpec(
            num_scalar_prefetch=1, grid=(1,), in_specs=[ANY] * (first - 1 + extra), out_specs=[ANY] * len(outs) + [TOKEN_SPEC],
            scratch_shapes=[pltpu.VMEM((total, d), BF16), pltpu.VMEM((d, full), BF16), pltpu.VMEM((total, HEAD), F32), pltpu.VMEM((total, HEAD), F32),
                            pltpu.VMEM((total, full), F32), pltpu.VMEM((heads, total, HEAD), BF16), pltpu.VMEM((total, HEAD), BF16),
                            pltpu.VMEM((total, HEAD), BF16), pltpu.SemaphoreType.DMA((10 * n + 12,))]),
        out_shape=outs + [TOKEN],
        input_output_aliases={first + i: len(outs) - extra + i for i in range(extra)},
        compiler_params=_params(),
        cost_estimate=_cost(total * d * full),
        name="project",
    )(me, dep, *pieces, *weights, cos, sin, *before, *through)


def _by_seen(me, dep, *refs, keys, extra):
    n = len(keys)
    pieces, wo, (out_hbm, g_hbm, tok, g_s, w_s, acc, stage, sem) = refs[:n], refs[n], refs[n + 1 + extra :]
    tok[...] = jnp.zeros_like(tok)
    rows, tokens = _rows(n), [pl.ds(_at(me, key), HALF) for key in keys]
    copies, parts = _Copies(sem), _parts(g_s.shape[1])
    loads = [copies.start([(p.at[:, part], g_s.at[r, part]) for p, r in zip(pieces, rows)] + [(wo.at[:, part], w_s.at[:, part])]) for part in parts]
    for c, part in enumerate(parts):
        _wait(loads[c])
        if part is parts[-1]:
            stores = copies.start([(g_s.at[r, :], g_hbm.at[there, :]) for r, there in zip(rows, tokens)])
        got = _dot(w_s[:, part], g_s[:, part], 1, 1)
        acc[...] = got if c == 0 else acc[...] + got
    stage[...] = acc[...].astype(BF16)
    _wait(stores + copies.start([(stage.at[:, r], out_hbm.at[:, there]) for r, there in zip(rows, tokens)]))


def by_seen(dep, me, pieces, keys, wo, rows, before):
    width, d = wo.shape
    n, extra = len(pieces), len(before)
    total = n * HALF
    return pl.pallas_call(
        functools.partial(_by_seen, keys=keys, extra=extra),
        grid_spec=pltpu.PrefetchScalarGridSpec(
            num_scalar_prefetch=1, grid=(1,), in_specs=[ANY] * (n + 2 + extra), out_specs=[ANY, ANY, TOKEN_SPEC],
            scratch_shapes=[pltpu.VMEM((total, d), BF16), pltpu.VMEM((width, d), BF16), pltpu.VMEM((width, total), F32), pltpu.VMEM((width, total), BF16),
                            pltpu.SemaphoreType.DMA((6 * n + 4,))]),
        out_shape=[jax.ShapeDtypeStruct((width, rows), BF16), jax.ShapeDtypeStruct((rows, d), BF16), TOKEN],
        input_output_aliases={3 + n + i: i for i in range(extra)},
        compiler_params=_params(),
        cost_estimate=_cost(total * d * width),
        name="by_seen",
    )(me, dep, *pieces, wo, *before)


def _attend(me, dep, q_ref, k_ref, v_ref, o_ref, lse_ref, tok, top_s, mix_s, gap_s, *, scale, bq, bk):
    g, d = q_ref.shape[0], q_ref.shape[2]
    iq = pl.program_id(0)
    e = scale * LOG2E

    @pl.when(iq == 0)
    def _():
        tok[...] = jnp.zeros_like(tok)
        gap_s[...] = lax.broadcasted_iota(jnp.int32, (bk, bq), 1) - lax.broadcasted_iota(jnp.int32, (bk, bq), 0)

    top_s[...] = jnp.full_like(top_s, NEG)
    mix_s[...] = jnp.zeros_like(mix_s)
    ones = jnp.ones((8, bk), BF16)

    def block(j, masked):
        here = pl.ds(pl.multiple_of(j * bk, bk), bk)
        scores = [_dot(k_ref[here, :], q_ref[n], 1, 1) for n in range(g)]
        ok = gap_s[...] >= j * bk - iq * bq if masked else None
        weights, keeps = [], []
        for n, s in enumerate(scores):
            if masked:
                s = jnp.where(ok, s, HIDDEN)
            old = top_s[n : n + 1, :]
            top = jnp.maximum(old, s.max(axis=0, keepdims=True))
            top_s[n : n + 1, :] = top
            weights.append(jnp.exp2((s - top) * e).astype(BF16))
            keeps.append(jnp.exp2((old - top) * e))
        values = jnp.concatenate([v_ref[here, :].T, ones], axis=0)
        for n, (p, keep) in enumerate(zip(weights, keeps)):
            mix_s[n] = mix_s[n] * keep + _dot(values, p, 1, 0)

    whole, last = lax.div(iq * bq, bk), lax.div(iq * bq + bq + bk - 1, bk)
    lax.fori_loop(0, whole, lambda j, _: block(j, False), None)
    lax.fori_loop(whole, last, lambda j, _: block(j, True), None)
    for n in range(g):
        total = mix_s[n, d : d + 1, :]
        o_ref[n] = (mix_s[n, :d, :] * (1 / total)).astype(BF16)
        lse_ref[n : n + 1, :] = top_s[n : n + 1, :] * scale + jnp.log(total)


def attend(dep, me, q, k, v, bq=512, bk=512):
    g, rows, d = q.shape
    whole = _whole(rows, d)
    return pl.pallas_call(
        functools.partial(_attend, scale=d**-0.5, bq=bq, bk=bk),
        grid_spec=pltpu.PrefetchScalarGridSpec(
            num_scalar_prefetch=1, grid=(rows // bq,),
            in_specs=[ANY, pl.BlockSpec((g, bq, d), lambda i, _: (0, i, 0)), whole, whole],
            out_specs=[pl.BlockSpec((g, d, bq), lambda i, _: (0, 0, i)), pl.BlockSpec((g, bq), lambda i, _: (0, i)),
                       TOKEN_SPEC],
            scratch_shapes=[pltpu.VMEM((g, bq), F32), pltpu.VMEM((g, d + 8, bq), F32), pltpu.VMEM((bk, bq), jnp.int32)]),
        out_shape=[jax.ShapeDtypeStruct((g, d, rows), BF16), jax.ShapeDtypeStruct((g, rows), F32), TOKEN],
        compiler_params=_params(),
        cost_estimate=_cost(2 * g * rows * rows * d),
        name="attend",
    )(me, dep, q, k, v)


def _chip(me, i, rs):
    r = rs[0]
    for n in range(1, len(rs)):
        r = jnp.where(i == n, rs[n], r)
    return (me[0] ^ r) // 2


def _back(me, dep, q_ref, k_ref, v_ref, do_ref, o_ref, lse_ref, cos, sin, *refs, scale, bq, bk, first, last, rs):
    g, d = q_ref.shape[0], q_ref.shape[2]
    if not first:
        dk_in, dv_in, refs = refs[0], refs[1], refs[2 + (2):]
    if last:
        dq_ref, dqt_ref, dkv_ref, dkvt_ref, tok, dq_s, gap_s, dk_s, dv_s = refs
    else:
        dq_ref, dqt_ref, dk_s, dv_s, tok, dq_s, gap_s = refs
    i = pl.program_id(0)
    iq = _chip(me, i, rs)
    e = scale * LOG2E
    half = d // 2

    @pl.when(i == 0)
    def _():
        tok[...] = jnp.zeros_like(tok)
        gap_s[...] = lax.broadcasted_iota(jnp.int32, (bk, bq), 1) - lax.broadcasted_iota(jnp.int32, (bk, bq), 0)
        if first:
            dk_s[...] = jnp.zeros_like(dk_s)
            dv_s[...] = jnp.zeros_like(dv_s)
        else:
            dk_s[...] = dk_in[...]
            dv_s[...] = dv_in[...]

    dq_s[...] = jnp.zeros_like(dq_s)
    lses = [lse_ref[n : n + 1, :] * LOG2E for n in range(g)]
    deltas = [(do_ref[n].astype(F32) * o_ref[n].astype(F32)).sum(0, keepdims=True) for n in range(g)]

    def block(j, masked):
        here = pl.ds(pl.multiple_of(j * bk, bk), bk)
        scores = [_dot(k_ref[here, :], q_ref[n], 1, 1) for n in range(g)]
        dps = [_dot(v_ref[here, :], do_ref[n], 1, 0) for n in range(g)]
        ok = gap_s[...] >= j * bk - iq * bq if masked else None
        kt = k_ref[here, :].T
        for n in range(g):
            p = jnp.exp2(scores[n] * e - lses[n])
            if masked:
                p = jnp.where(ok, p, 0.0)
            ds = (p * (dps[n] - deltas[n])).astype(BF16)
            dv_s[here, :] += _dot(p.astype(BF16), do_ref[n], 1, 1)
            dk_s[here, :] += _dot(ds, q_ref[n], 1, 0)
            dq_s[n] += _dot(kt, ds, 1, 0)

    whole, end = lax.div(iq * bq, bk), lax.div(iq * bq + bq + bk - 1, bk)
    lax.fori_loop(0, whole, lambda j, _: block(j, False), None)
    lax.fori_loop(whole, end, lambda j, _: block(j, True), None)

    def unturned(t, c, s):
        t = t.astype(BF16).astype(F32)
        a, b = t[:half], t[half:]
        return jnp.concatenate([a * c + b * s, b * c - a * s], axis=0)

    at = pl.ds(pl.multiple_of(iq * bq, bq), bq)
    for n in range(g):
        t = unturned(dq_s[n] * scale, cos[:, at], sin[:, at])
        dqt_ref[n * d : (n + 1) * d, :] = t.astype(BF16)
        dq_ref[:, n * d : (n + 1) * d] = t.T.astype(BF16)

    if last:
        @pl.when(i == len(rs) - 1)
        def _():
            t = unturned((dk_s[...] * scale).T, cos[...], sin[...])
            dkvt_ref[:d, :] = t.astype(BF16)
            dkv_ref[:, :d] = t.T.astype(BF16)
            dkvt_ref[d:, :] = dv_s[...].T.astype(BF16)
            dkv_ref[:, d:] = dv_s[...].astype(BF16)


def back(dep, me, rs, q, k, v, do_t, out_t, lse, cos_t, sin_t, before, last, bk=512):
    g, rows, d = q.shape
    first, bq = before is None, rows // 4
    here = lambda i, me: _chip(me, i, rs)
    whole = _whole(rows, d)
    table = _whole(d // 2, rows)
    across = pl.BlockSpec((g, d, bq), lambda i, me: (0, 0, here(i, me)))
    specs = [ANY, pl.BlockSpec((g, bq, d), lambda i, me: (0, here(i, me), 0)), whole, whole, across, across, pl.BlockSpec((g, bq), lambda i, me: (0, here(i, me))), table, table]
    given = [dep, q, k, v, do_t, out_t, lse, cos_t, sin_t]
    aliases = {}
    if not first:
        specs += [whole, whole, ANY, ANY]
        given += [before[2], before[3], before[0], before[1]]
        aliases = {2 + 10: 0, 2 + 11: 1}
    outs = [jax.ShapeDtypeStruct((rows, g * d), BF16), jax.ShapeDtypeStruct((g * d, rows), BF16)]
    out_specs = [pl.BlockSpec((bq, g * d), lambda i, me: (here(i, me), 0)), pl.BlockSpec((g * d, bq), lambda i, me: (0, here(i, me)))]
    scratch = [pltpu.VMEM((g, d, bq), F32), pltpu.VMEM((bk, bq), jnp.int32)]
    if last:
        outs += [jax.ShapeDtypeStruct((rows, 2 * d), BF16), jax.ShapeDtypeStruct((2 * d, rows), BF16)]
        out_specs += [_whole(rows, 2 * d), _whole(2 * d, rows)]
        scratch += [pltpu.VMEM((rows, d), F32)] * 2
    else:
        outs += [jax.ShapeDtypeStruct((rows, d), F32)] * 2
        out_specs += [whole, whole]
    return pl.pallas_call(
        functools.partial(_back, scale=d**-0.5, bq=bq, bk=bk, first=first, last=last, rs=rs),
        grid_spec=pltpu.PrefetchScalarGridSpec(num_scalar_prefetch=1, grid=(len(rs),), in_specs=specs,
                                               out_specs=out_specs + [pl.BlockSpec((8, 128), lambda i, b: (0, 0))], scratch_shapes=scratch),
        out_shape=outs + [TOKEN],
        input_output_aliases=aliases,
        compiler_params=_params(),
        cost_estimate=_cost(4 * g * len(rs) * bq * rows * d),
        name="back",
    )(me, *given)


def _by_states(me, dep, dq, dkv, wq, wk, wv, *refs, keys, adds, groups):
    n, many = len(keys), len(groups)
    added, outs, tok, refs = refs[: len(adds)], refs[len(adds) : len(adds) + many], refs[len(adds) + many], refs[len(adds) + many + 1 :]
    stages, (lhs_s, w_s, add_s, sem) = refs[:many], refs[many:]
    tok[...] = jnp.zeros_like(tok)
    rows, cols = _rows(max(n, len(adds))), dq.shape[1]
    copies, parts = _Copies(sem), _parts(w_s.shape[0])
    loads = []
    for key, r in zip(keys, rows):
        there = pl.ds(_at(me, key), HALF)
        loads += copies.start([(dq.at[there, :], lhs_s.at[r, :cols]), (dkv.at[there, :], lhs_s.at[r, cols:])])
    loads = [(loads if c == 0 else []) + copies.start(_stacked((wq, wk, wv), w_s, part)
                                                      + [(a.at[_rows(row + 1)[row], part], add_s.at[r, part]) for a, (_, row), r in zip(added, adds, rows)])
             for c, part in enumerate(parts)]
    place, stores = [(o, r) for o, k in enumerate(groups) for r in _rows(k)], []
    for c, part in enumerate(parts):
        _wait(loads[c])
        got = _dot(lhs_s[...], w_s[part, :], 1, 1)
        for i, (o, r) in enumerate(place):
            t = got[i * HALF : (i + 1) * HALF]
            for (target, _), mine in zip(adds, rows):
                if target == i:
                    t = t + add_s[mine, part].astype(F32)
            stages[o][r, part] = t.astype(stages[o].dtype)
        stores += copies.start([(stage.at[:, part], out.at[:, part]) for stage, out in zip(stages, outs)])
    _wait(stores)


def by_states(dep, me, keys, dq, dkv, weights, adds, groups, dtypes):
    d, n, many, full = weights[0].shape[0], len(keys), len(adds), sum(w.shape[1] for w in weights)
    shapes = [((k * HALF, d), t) for k, t in zip(groups, dtypes)]
    return pl.pallas_call(
        functools.partial(_by_states, keys=keys, adds=[(i, row) for i, _, row in adds], groups=groups),
        grid_spec=pltpu.PrefetchScalarGridSpec(
            num_scalar_prefetch=1, grid=(1,), in_specs=[ANY] * (6 + many), out_specs=[ANY] * len(groups) + [TOKEN_SPEC],
            scratch_shapes=[pltpu.VMEM(*s) for s in shapes] + [pltpu.VMEM((n * HALF, full), BF16), pltpu.VMEM((d, full), BF16),
                                                               pltpu.VMEM((max(many, 1) * HALF, d), BF16),
                                                               pltpu.SemaphoreType.DMA((2 * n + 4 * (3 + many + len(groups)),))]),
        out_shape=[jax.ShapeDtypeStruct(*s) for s in shapes] + [TOKEN],
        compiler_params=_params(),
        cost_estimate=_cost(n * HALF * d * full),
        name="by_states",
    )(me, dep, dq, dkv, *weights, *(a for _, a, _ in adds))


def _by_qkv(me, dep, a, dqt, dkvt, *refs, extra):
    gq, gk, gv, tok, r_s = refs[extra:]
    tok[...] = jnp.zeros_like(tok)
    wide = dqt.shape[0]
    r_s[:wide] = _dot(dqt[...], a[...], 1, 0)
    r_s[wide:] = _dot(dkvt[...], a[...], 1, 0)
    for h in range(r_s.shape[0] // HEAD):
        t = r_s[h * HEAD : (h + 1) * HEAD].T.astype(BF16)
        if h * HEAD < wide:
            gq[:, h * HEAD : (h + 1) * HEAD] = t
        else:
            (gk if h * HEAD == wide else gv)[...] = t


def by_qkv(dep, me, a, dqt, dkvt, lo, hi, before, bm=1024):
    (rows, d), width, extra = a.shape, dqt.shape[0], len(before)
    return pl.pallas_call(
        functools.partial(_by_qkv, extra=extra),
        grid_spec=pltpu.PrefetchScalarGridSpec(
            num_scalar_prefetch=1, grid=(hi - lo,),
            in_specs=[ANY, pl.BlockSpec((rows, bm), lambda j, _: (0, lo + j)), _whole(*dqt.shape), _whole(*dkvt.shape)] + [ANY] * extra,
            out_specs=[pl.BlockSpec((bm, w), lambda j, _: (lo + j, 0)) for w in (width, HEAD, HEAD)] + [TOKEN_SPEC],
            scratch_shapes=[pltpu.VMEM((width + 2 * HEAD, bm), F32)]),
        out_shape=[jax.ShapeDtypeStruct((d, w), BF16) for w in (width, HEAD, HEAD)] + [TOKEN],
        input_output_aliases={5 + i: i for i in range(extra)},
        compiler_params=_params(),
        cost_estimate=_cost(rows * (hi - lo) * bm * (width + 2 * HEAD)),
        name="by_qkv",
    )(me, dep, a, dqt, dkvt, *before)


def _by_wo(me, dep, g, seen_t, out, tok):
    tok[...] = jnp.zeros_like(tok)
    out[...] = _dot(seen_t[...], g[...], 1, 0).astype(BF16)


def by_wo(dep, me, g, seen_t, bn=1024):
    (rows, d), width = g.shape, seen_t.shape[0]
    return pl.pallas_call(
        _by_wo,
        grid_spec=pltpu.PrefetchScalarGridSpec(
            num_scalar_prefetch=1, grid=(d // bn,), in_specs=[ANY, pl.BlockSpec((rows, bn), lambda j, _: (0, j)), _whole(width, rows)],
            out_specs=[pl.BlockSpec((width, bn), lambda j, _: (0, j)), TOKEN_SPEC]),
        out_shape=[jax.ShapeDtypeStruct((width, d), BF16), TOKEN],
        compiler_params=_params(),
        cost_estimate=_cost(rows * d * width),
        name="by_wo",
    )(me, dep, g, seen_t)


def _finish(me, dep, own, r40, r41, r20, r21, x, dy, gain, by_x, by_gain):
    i = pl.program_id(0)
    early = i < pl.num_programs(0) // 2
    sent = [jnp.where(early, a[...], b[...]).astype(F32) for a, b in ((r40, r41), (r20, r21))]
    da, wide = own[...] + sent[0] + sent[1], x[...].astype(F32)
    scale = lax.rsqrt(jnp.mean(wide * wide, -1, keepdims=True) + 1e-6)
    unit, inner = wide * scale, da * gain[...].astype(F32)
    by_x[...] = (dy[...].astype(F32) + scale * (inner - unit * jnp.mean(inner * unit, -1, keepdims=True))).astype(BF16)
    part = jnp.sum(da * unit, 0, keepdims=True)
    by_gain[...] = jnp.where(i == 0, part, by_gain[...] + part)


def finish(dep, me, own, sent, x, dy, gain, block=64):
    rows, d = x.shape
    steps = rows // block
    each = pl.BlockSpec((block, d), lambda i, _: (i, 0))
    halves = [pl.BlockSpec((block, d), lambda i, _: (jnp.minimum(i, steps // 2 - 1), 0)), pl.BlockSpec((block, d), lambda i, _: (jnp.maximum(i - steps // 2, 0), 0))]
    return pl.pallas_call(
        _finish,
        grid_spec=pltpu.PrefetchScalarGridSpec(
            num_scalar_prefetch=1, grid=(steps,), in_specs=[ANY, each, *halves, *halves, each, each, _whole(1, d)], out_specs=[each, _whole(1, d)]),
        out_shape=[jax.ShapeDtypeStruct((rows, d), BF16), jax.ShapeDtypeStruct((1, d), F32)],
        compiler_params=_params(),
        cost_estimate=_cost(rows * d * HEAD),
        name="finish",
    )(me, dep, own, *sent, x, dy, gain.reshape(1, d))


def swap(value, r):
    return lax.ppermute(value, "tp", [(i, i ^ r) for i in range(8)])


def normed(x, gain):
    wide = x.astype(F32)
    scale = lax.rsqrt(jnp.mean(wide * wide, -1, keepdims=True) + 1e-6)
    return (wide * scale * gain.astype(F32)).astype(BF16)


def gather(halves):
    got = {(0, i): t for i, t in enumerate(halves)}

    def send(r, i, by):
        got[r, i] = swap(got[r ^ by, i], by)

    for r, i in ((4, 0), (2, 1), (1, 0), (1, 1), (4, 1), (2, 0)):
        send(r, i, r)
    send(6, 0, 2)
    send(6, 1, 4)
    for r, i in ((4, 0), (2, 1), (4, 1), (2, 0), (6, 0), (6, 1)):
        send(r ^ 1, i, 1)
    return got


def solution(mesh):
    def step(x, dy, gain, wq, wk, wv, wo):
        me = lax.axis_index("tp").astype(jnp.int32).reshape(1)
        rows, weights = x.shape[0] * 8, [wq, wk, wv]
        angle = jnp.arange(rows).astype(F32)[:, None] * THETA ** (-jnp.arange(HEAD // 2, dtype=F32) / (HEAD // 2))
        cos, sin = jnp.cos(angle), jnp.sin(angle)
        cos_w, sin_w = jnp.concatenate([cos, cos], 1), jnp.concatenate([-sin, sin], 1)
        cos_t, sin_t = cos.T, sin.T
        order = [[(0, 0), (0, 1), (1, 0), (1, 1)], [(4, 0), (5, 0), (2, 1), (3, 1)], [(4, 1), (5, 1), (2, 0), (3, 0)], [(6, 0), (7, 0), (6, 1), (7, 1)]]

        a = gather([normed(x[:HALF], gain), normed(x[HALF:], gain)])

        def projected(n, token, before, through=()):
            return project(token, me, [a[key] for key in order[n]], order[n], weights, cos_w, sin_w, before, through)

        def seen_grad(n, token, before):
            return by_seen(token, me, [g[key] for key in order[n]], order[n], wo, rows, before)

        *known, token = projected(0, jnp.zeros(TOKEN.shape, F32), [])
        *known, g0, g1, token = projected(1, token, known, [dy[:HALF], dy[HALF:]])
        g = gather([g0, g1])
        *known, token = projected(2, token, known)
        *grads, token = seen_grad(0, token, [])
        *known, token = projected(3, token, known)
        q, k, v, states = known
        out, lse, token = attend(token, me, q, k, v)
        heads = q.shape[0]

        def attention_back(rs, token, before, last):
            return back(token, me, rs, q, k, v, grads[0].reshape(heads, HEAD, rows), out, lse, cos_t, sin_t, before, last)

        *sums, token = attention_back((0,), token, None, False)
        *grads, token = seen_grad(1, token, grads)
        *grads, token = seen_grad(2, token, grads)
        *sums, token = attention_back((4, 2), token, sums, False)
        *grads, token = seen_grad(3, token, grads)
        dq, dq_t, dkv, dkv_t, token = attention_back((6,), token, sums, True)

        both = lambda r: [(r, 0), (r, 1)]

        def term(token, keys, groups, adds=(), dtypes=(BF16,) * 4):
            return by_states(token, me, keys, dq, dkv, weights, adds, groups, dtypes)

        t7, token = term(token, both(7), [2])
        p6 = swap(t7, 1)
        t5, t3, token = term(token, both(5) + both(3), [2, 2])
        p4, p2 = swap(t5, 1), swap(t3, 1)
        s60, s61, token = term(token, both(6), [1, 1], [(0, p6, 0), (1, p6, 1)])
        far2, far4 = swap(s60, 4), swap(s61, 2)
        s40, s21, t1, token = term(token, [(4, 0), (2, 1)] + both(1), [1, 1, 2], [(0, p4, 0), (1, p2, 1)])
        r40, r21 = swap(s40, 4), swap(s21, 2)
        p0 = swap(t1, 1)
        *by_w, token = by_qkv(token, me, states, dq_t, dkv_t, 0, 2, [])
        s41, s20, own, token = term(token, [(4, 1), (2, 0)] + both(0), [1, 1, 2],
                                    [(0, p4, 1), (0, far4, 0), (1, p2, 0), (1, far2, 0), (2, p0, 0), (3, p0, 1)], (BF16, BF16, F32))
        r41, r20 = swap(s41, 4), swap(s20, 2)
        by_o, token = by_wo(token, me, grads[1], out.reshape(heads * HEAD, rows))
        *by_w, token = by_qkv(token, me, states, dq_t, dkv_t, 2, 6, by_w)
        *by_w, _ = by_qkv(token, me, states, dq_t, dkv_t, 6, 7, by_w)
        by_x, by_gain = finish(token, me, own, [r40, r41, r20, r21], x, dy, gain)
        t = [by_gain] + [swap(by_gain, r) for r in range(1, 8)]
        while len(t) > 1:
            t = [t[i] + t[i + 1] for i in range(0, len(t), 2)]
        return (by_x, t[0], *by_w, by_o)

    tokens, columns = P(("dp", "tp"), None), P(None, "tp")
    return jax.shard_map(
        step,
        mesh=mesh,
        in_specs=(tokens, tokens, P(None), columns, columns, columns, P("tp", None)),
        out_specs=(tokens, P("dp", None), P("dp", "tp"), P("dp", "tp"), P("dp", "tp"), P(("dp", "tp"), None)),
        check_vma=False,
    )
```

```python
import functools

import jax
import jax.numpy as jnp
from jax import lax
from jax.experimental import pallas as pl
from jax.experimental.pallas import tpu as pltpu
from jax.sharding import PartitionSpec as P


HEAD = 128
THETA = 10000
NEG = -1e30
HIDDEN = 2 * NEG
LOG2E = 1.4426950408889634
VMEM = 60 * 2**20
F32, BF16 = jnp.float32, jnp.bfloat16
ANY = pl.BlockSpec(memory_space=pl.ANY)
TOKEN = jax.ShapeDtypeStruct((8, 128), F32)
TOKEN_SPEC = pl.BlockSpec(TOKEN.shape, lambda i, _: (0, 0))


def _dot(a, b, ca, cb):
    return lax.dot_general(a, b, (((ca,), (cb,)), ((), ())), preferred_element_type=F32)


def _params():
    return pltpu.CompilerParams(dimension_semantics=("arbitrary",), vmem_limit_bytes=VMEM)


def _cost(products):
    return pl.CostEstimate(flops=2 * products, bytes_accessed=products // 64, transcendentals=0)


def _whole(*shape):
    return pl.BlockSpec(shape, lambda i, _: (0, 0))


HALF = 128


def _at(me, key):
    return pl.multiple_of(((me[0] ^ key[0]) * 2 + key[1]) * HALF, HALF)


def _rows(n):
    return [pl.ds(i * HALF, HALF) for i in range(n)]


def _parts(size, cuts=(0, 1, 3, 5, 7)):
    return [pl.ds(lo * size // 7, (hi - lo) * size // 7) for lo, hi in zip(cuts, cuts[1:])]


class _Copies:
    def __init__(self, sem):
        self.sem, self.used = sem, 0

    def start(self, pairs):
        made = []
        for src, dst in pairs:
            made.append(pltpu.make_async_copy(src, dst, self.sem.at[self.used]))
            made[-1].start()
            self.used += 1
        return made


def _wait(copies):
    for c in copies:
        c.wait()


def _stacked(weights, w_s, part):
    at, pairs = 0, []
    for w in weights:
        pairs.append((w.at[part, :], w_s.at[part, at : at + w.shape[1]]))
        at += w.shape[1]
    return pairs


def _project(me, dep, *refs, keys, heads, extra, through):
    n = len(keys)
    pieces, (wq, wk, wv, cos, sin), refs = refs[:n], refs[n : n + 5], refs[n + 5 + extra :]
    q_hbm, k_hbm, v_hbm, a_hbm = refs[:4]
    tok, a_s, w_s, cos_s, sin_s, acc, q_s, k_s, v_s, sem = refs[4 + through :]
    tok[...] = jnp.zeros_like(tok)
    rows, tokens = _rows(n), [pl.ds(_at(me, key), HALF) for key in keys]
    copies, parts = _Copies(sem), _parts(a_s.shape[1])
    loads = [copies.start([(p.at[:, part], a_s.at[r, part]) for p, r in zip(pieces, rows)] + _stacked((wq, wk, wv), w_s, part)) for part in parts]
    loads[-1] += copies.start([(t.at[there, :], s.at[r, :]) for t, s in ((cos, cos_s), (sin, sin_s)) for r, there in zip(rows, tokens)])
    for c, part in enumerate(parts):
        _wait(loads[c])
        if part is parts[-1]:
            stores = copies.start([(a_s.at[r, :], a_hbm.at[there, :]) for r, there in zip(rows, tokens)])
        got = _dot(a_s[:, part], w_s[part, :], 1, 0)
        acc[...] = got if c == 0 else acc[...] + got
    for h in range(heads + 2):
        t = acc[:, h * HEAD : (h + 1) * HEAD].astype(BF16)
        if h <= heads:
            t = t.astype(F32)
            t = (t * cos_s[...] + pltpu.roll(t, HEAD // 2, 1) * sin_s[...]).astype(BF16)
        if h < heads:
            q_s[h] = t
        else:
            (k_s if h == heads else v_s)[...] = t
    for r, there in zip(rows, tokens):
        stores += copies.start([(q_s.at[:, r, :], q_hbm.at[:, there, :]), (k_s.at[r, :], k_hbm.at[there, :]), (v_s.at[r, :], v_hbm.at[there, :])])
    _wait(stores)


def project(dep, me, pieces, keys, weights, cos, sin, before, through=()):
    (d, width), more = weights[0].shape, weights[1].shape[1]
    heads, rows, n, full = width // HEAD, cos.shape[0], len(pieces), width + 2 * more
    total, extra = n * HALF, len(before) + len(through)
    outs = [jax.ShapeDtypeStruct(s, BF16) for s in ((heads, rows, HEAD), (rows, HEAD), (rows, HEAD), (rows, d))]
    outs += [jax.ShapeDtypeStruct(t.shape, t.dtype) for t in through]
    first = 2 + n + 5
    return pl.pallas_call(
        functools.partial(_project, keys=keys, heads=heads, extra=extra, through=len(through)),
        grid_spec=pltpu.PrefetchScalarGridSpec(
            num_scalar_prefetch=1, grid=(1,), in_specs=[ANY] * (first - 1 + extra), out_specs=[ANY] * len(outs) + [TOKEN_SPEC],
            scratch_shapes=[pltpu.VMEM((total, d), BF16), pltpu.VMEM((d, full), BF16), pltpu.VMEM((total, HEAD), F32), pltpu.VMEM((total, HEAD), F32),
                            pltpu.VMEM((total, full), F32), pltpu.VMEM((heads, total, HEAD), BF16), pltpu.VMEM((total, HEAD), BF16),
                            pltpu.VMEM((total, HEAD), BF16), pltpu.SemaphoreType.DMA((10 * n + 12,))]),
        out_shape=outs + [TOKEN],
        input_output_aliases={first + i: len(outs) - extra + i for i in range(extra)},
        compiler_params=_params(),
        cost_estimate=_cost(total * d * full),
        name="project",
    )(me, dep, *pieces, *weights, cos, sin, *before, *through)


def _by_seen(me, dep, *refs, keys, extra):
    n = len(keys)
    pieces, wo, (out_hbm, g_hbm, tok, g_s, w_s, acc, stage, sem) = refs[:n], refs[n], refs[n + 1 + extra :]
    tok[...] = jnp.zeros_like(tok)
    rows, tokens = _rows(n), [pl.ds(_at(me, key), HALF) for key in keys]
    copies, parts = _Copies(sem), _parts(g_s.shape[1])
    loads = [copies.start([(p.at[:, part], g_s.at[r, part]) for p, r in zip(pieces, rows)] + [(wo.at[:, part], w_s.at[:, part])]) for part in parts]
    for c, part in enumerate(parts):
        _wait(loads[c])
        if part is parts[-1]:
            stores = copies.start([(g_s.at[r, :], g_hbm.at[there, :]) for r, there in zip(rows, tokens)])
        got = _dot(w_s[:, part], g_s[:, part], 1, 1)
        acc[...] = got if c == 0 else acc[...] + got
    stage[...] = acc[...].astype(BF16)
    _wait(stores + copies.start([(stage.at[:, r], out_hbm.at[:, there]) for r, there in zip(rows, tokens)]))


def by_seen(dep, me, pieces, keys, wo, rows, before):
    width, d = wo.shape
    n, extra = len(pieces), len(before)
    total = n * HALF
    return pl.pallas_call(
        functools.partial(_by_seen, keys=keys, extra=extra),
        grid_spec=pltpu.PrefetchScalarGridSpec(
            num_scalar_prefetch=1, grid=(1,), in_specs=[ANY] * (n + 2 + extra), out_specs=[ANY, ANY, TOKEN_SPEC],
            scratch_shapes=[pltpu.VMEM((total, d), BF16), pltpu.VMEM((width, d), BF16), pltpu.VMEM((width, total), F32), pltpu.VMEM((width, total), BF16),
                            pltpu.SemaphoreType.DMA((6 * n + 4,))]),
        out_shape=[jax.ShapeDtypeStruct((width, rows), BF16), jax.ShapeDtypeStruct((rows, d), BF16), TOKEN],
        input_output_aliases={3 + n + i: i for i in range(extra)},
        compiler_params=_params(),
        cost_estimate=_cost(total * d * width),
        name="by_seen",
    )(me, dep, *pieces, wo, *before)


def _attend(me, dep, q_ref, k_ref, v_ref, o_ref, lse_ref, tok, top_s, mix_s, gap_s, *, scale, bq):
    g, d = q_ref.shape[0], q_ref.shape[2]
    iq = pl.program_id(0)
    e = scale * LOG2E

    @pl.when(iq == 0)
    def _():
        tok[...] = jnp.zeros_like(tok)
        gap_s[...] = lax.broadcasted_iota(jnp.int32, gap_s.shape, 1) - lax.broadcasted_iota(jnp.int32, gap_s.shape, 0)

    top_s[...] = jnp.full_like(top_s, NEG)
    mix_s[...] = jnp.zeros_like(mix_s)

    def block(first, keys, lo, masked):
        here, there = pl.ds(pl.multiple_of(first, keys), keys), pl.ds(lo, bq - lo)
        scores = [_dot(k_ref[here, :], q_ref[n, there, :], 1, 1) for n in range(g)]
        weights, keeps = [], []
        for n, s in enumerate(scores):
            if masked:
                s = jnp.where(gap_s[:keys, : bq - lo] >= 0, s, HIDDEN)
            old = top_s[n : n + 1, there]
            top = jnp.maximum(old, s.max(axis=0, keepdims=True))
            top_s[n : n + 1, there] = top
            weights.append(jnp.exp2((s - top) * e).astype(BF16))
            keeps.append(jnp.exp2((old - top) * e))
        values = jnp.concatenate([v_ref[here, :].T, jnp.ones((8, keys), BF16)], axis=0)
        for n, (p, keep) in enumerate(zip(weights, keeps)):
            mix_s[n, :, there] = mix_s[n, :, there] * keep + _dot(values, p, 1, 0)

    lax.fori_loop(0, iq, lambda j, _: block(j * bq, bq, 0, False), None)
    for lo in (0, bq // 2):
        block(iq * bq + lo, bq // 2, lo, True)
    for n in range(g):
        total = mix_s[n, d : d + 1, :]
        o_ref[n] = (mix_s[n, :d, :] * (1 / total)).astype(BF16)
        lse_ref[n : n + 1, :] = top_s[n : n + 1, :] * scale + jnp.log(total)


def attend(dep, me, q, k, v, bq=512):
    g, rows, d = q.shape
    whole = _whole(rows, d)
    return pl.pallas_call(
        functools.partial(_attend, scale=d**-0.5, bq=bq),
        grid_spec=pltpu.PrefetchScalarGridSpec(
            num_scalar_prefetch=1, grid=(rows // bq,),
            in_specs=[ANY, pl.BlockSpec((g, bq, d), lambda i, _: (0, i, 0)), whole, whole],
            out_specs=[pl.BlockSpec((g, d, bq), lambda i, _: (0, 0, i)), pl.BlockSpec((g, bq), lambda i, _: (0, i)),
                       TOKEN_SPEC],
            scratch_shapes=[pltpu.VMEM((g, bq), F32), pltpu.VMEM((g, d + 8, bq), F32), pltpu.VMEM((bq // 2, bq), jnp.int32)]),
        out_shape=[jax.ShapeDtypeStruct((g, d, rows), BF16), jax.ShapeDtypeStruct((g, rows), F32), TOKEN],
        compiler_params=_params(),
        cost_estimate=_cost(2 * g * rows * rows * d),
        name="attend",
    )(me, dep, q, k, v)


def _chip(me, i, rs):
    r = rs[0]
    for n in range(1, len(rs)):
        r = jnp.where(i == n, rs[n], r)
    return (me[0] ^ r) // 2


def _back(me, dep, q_ref, k_ref, v_ref, do_ref, o_ref, lse_ref, cos, sin, *refs, scale, bq, first, last, rs):
    g, d = q_ref.shape[0], q_ref.shape[2]
    if not first:
        dk_in, dv_in, refs = refs[0], refs[1], refs[2 + (2):]
    if last:
        dq_ref, dqt_ref, dkv_ref, dkvt_ref, tok, dq_s, gap_s, dk_s, dv_s = refs
    else:
        dq_ref, dqt_ref, dk_s, dv_s, tok, dq_s, gap_s = refs
    i = pl.program_id(0)
    iq = _chip(me, i, rs)
    e = scale * LOG2E
    half = d // 2

    @pl.when(i == 0)
    def _():
        tok[...] = jnp.zeros_like(tok)
        gap_s[...] = lax.broadcasted_iota(jnp.int32, gap_s.shape, 1) - lax.broadcasted_iota(jnp.int32, gap_s.shape, 0)
        if first:
            dk_s[...] = jnp.zeros_like(dk_s)
            dv_s[...] = jnp.zeros_like(dv_s)
        else:
            dk_s[...] = dk_in[...]
            dv_s[...] = dv_in[...]

    dq_s[...] = jnp.zeros_like(dq_s)
    lses = [lse_ref[n : n + 1, :] * LOG2E for n in range(g)]
    deltas = [(do_ref[n].astype(F32) * o_ref[n].astype(F32)).sum(0, keepdims=True) for n in range(g)]

    def block(first, keys, lo, masked):
        here, there = pl.ds(pl.multiple_of(first, keys), keys), pl.ds(lo, bq - lo)
        scores = [_dot(k_ref[here, :], q_ref[n, there, :], 1, 1) for n in range(g)]
        dps = [_dot(v_ref[here, :], do_ref[n, :, there], 1, 0) for n in range(g)]
        kt = k_ref[here, :].T
        for n in range(g):
            p = jnp.exp2(scores[n] * e - lses[n][:, lo:])
            if masked:
                p = jnp.where(gap_s[:keys, : bq - lo] >= 0, p, 0.0)
            ds = (p * (dps[n] - deltas[n][:, lo:])).astype(BF16)
            dv_s[here, :] += _dot(p.astype(BF16), do_ref[n, :, there], 1, 1)
            dk_s[here, :] += _dot(ds, q_ref[n, there, :], 1, 0)
            dq_s[n, :, there] += _dot(kt, ds, 1, 0)

    lax.fori_loop(0, iq, lambda j, _: block(j * bq, bq, 0, False), None)
    for lo in (0, bq // 2):
        block(iq * bq + lo, bq // 2, lo, True)

    def unturned(t, c, s):
        t = t.astype(BF16).astype(F32)
        a, b = t[:half], t[half:]
        return jnp.concatenate([a * c + b * s, b * c - a * s], axis=0)

    at = pl.ds(pl.multiple_of(iq * bq, bq), bq)
    for n in range(g):
        t = unturned(dq_s[n] * scale, cos[:, at], sin[:, at])
        dqt_ref[n * d : (n + 1) * d, :] = t.astype(BF16)
        dq_ref[:, n * d : (n + 1) * d] = t.T.astype(BF16)

    if last:
        @pl.when(i == len(rs) - 1)
        def _():
            t = unturned((dk_s[...] * scale).T, cos[...], sin[...])
            dkvt_ref[:d, :] = t.astype(BF16)
            dkv_ref[:, :d] = t.T.astype(BF16)
            dkvt_ref[d:, :] = dv_s[...].T.astype(BF16)
            dkv_ref[:, d:] = dv_s[...].astype(BF16)


def back(dep, me, rs, q, k, v, do_t, out_t, lse, cos_t, sin_t, before, last):
    g, rows, d = q.shape
    first, bq = before is None, rows // 4
    here = lambda i, me: _chip(me, i, rs)
    whole = _whole(rows, d)
    table = _whole(d // 2, rows)
    across = pl.BlockSpec((g, d, bq), lambda i, me: (0, 0, here(i, me)))
    specs = [ANY, pl.BlockSpec((g, bq, d), lambda i, me: (0, here(i, me), 0)), whole, whole, across, across, pl.BlockSpec((g, bq), lambda i, me: (0, here(i, me))), table, table]
    given = [dep, q, k, v, do_t, out_t, lse, cos_t, sin_t]
    aliases = {}
    if not first:
        specs += [whole, whole, ANY, ANY]
        given += [before[2], before[3], before[0], before[1]]
        aliases = {2 + 10: 0, 2 + 11: 1}
    outs = [jax.ShapeDtypeStruct((rows, g * d), BF16), jax.ShapeDtypeStruct((g * d, rows), BF16)]
    out_specs = [pl.BlockSpec((bq, g * d), lambda i, me: (here(i, me), 0)), pl.BlockSpec((g * d, bq), lambda i, me: (0, here(i, me)))]
    scratch = [pltpu.VMEM((g, d, bq), F32), pltpu.VMEM((bq // 2, bq), jnp.int32)]
    if last:
        outs += [jax.ShapeDtypeStruct((rows, 2 * d), BF16), jax.ShapeDtypeStruct((2 * d, rows), BF16)]
        out_specs += [_whole(rows, 2 * d), _whole(2 * d, rows)]
        scratch += [pltpu.VMEM((rows, d), F32)] * 2
    else:
        outs += [jax.ShapeDtypeStruct((rows, d), F32)] * 2
        out_specs += [whole, whole]
    return pl.pallas_call(
        functools.partial(_back, scale=d**-0.5, bq=bq, first=first, last=last, rs=rs),
        grid_spec=pltpu.PrefetchScalarGridSpec(num_scalar_prefetch=1, grid=(len(rs),), in_specs=specs,
                                               out_specs=out_specs + [pl.BlockSpec((8, 128), lambda i, b: (0, 0))], scratch_shapes=scratch),
        out_shape=outs + [TOKEN],
        input_output_aliases=aliases,
        compiler_params=_params(),
        cost_estimate=_cost(4 * g * len(rs) * bq * rows * d),
        name="back",
    )(me, *given)


def _by_states(me, dep, dq, dkv, wq, wk, wv, *refs, keys, adds, groups):
    n, many = len(keys), len(groups)
    added, outs, tok, refs = refs[: len(adds)], refs[len(adds) : len(adds) + many], refs[len(adds) + many], refs[len(adds) + many + 1 :]
    stages, (lhs_s, w_s, add_s, sem) = refs[:many], refs[many:]
    tok[...] = jnp.zeros_like(tok)
    rows, cols = _rows(n + len(adds)), dq.shape[1]
    copies, parts = _Copies(sem), _parts(w_s.shape[0])
    loads = []
    for key, r in zip(keys, rows):
        there = pl.ds(_at(me, key), HALF)
        loads += copies.start([(dq.at[there, :], lhs_s.at[r, :cols]), (dkv.at[there, :], lhs_s.at[r, cols:])])
    loads = [(loads if c == 0 else []) + copies.start(_stacked((wq, wk, wv), w_s, part)
                                                      + [(a.at[_rows(row + 1)[row], part], add_s.at[r, part]) for a, (_, row), r in zip(added, adds, rows)])
             for c, part in enumerate(parts)]
    place, stores = [(o, r) for o, k in enumerate(groups) for r in _rows(k)], []
    for c, part in enumerate(parts):
        _wait(loads[c])
        got = _dot(lhs_s[...], w_s[part, :], 1, 1)
        for i, (o, r) in enumerate(place):
            t = got[i * HALF : (i + 1) * HALF]
            for (target, _), mine in zip(adds, rows):
                if target == i:
                    t = t + add_s[mine, part].astype(F32)
            stages[o][r, part] = t.astype(stages[o].dtype)
        stores += copies.start([(stage.at[:, part], out.at[:, part]) for stage, out in zip(stages, outs)])
    _wait(stores)


def by_states(dep, me, keys, dq, dkv, weights, adds, groups, dtypes):
    d, n, many, full = weights[0].shape[0], len(keys), len(adds), sum(w.shape[1] for w in weights)
    shapes = [((k * HALF, d), t) for k, t in zip(groups, dtypes)]
    return pl.pallas_call(
        functools.partial(_by_states, keys=keys, adds=[(i, row) for i, _, row in adds], groups=groups),
        grid_spec=pltpu.PrefetchScalarGridSpec(
            num_scalar_prefetch=1, grid=(1,), in_specs=[ANY] * (6 + many), out_specs=[ANY] * len(groups) + [TOKEN_SPEC],
            scratch_shapes=[pltpu.VMEM(*s) for s in shapes] + [pltpu.VMEM((n * HALF, full), BF16), pltpu.VMEM((d, full), BF16),
                                                               pltpu.VMEM((max(many, 1) * HALF, d), BF16),
                                                               pltpu.SemaphoreType.DMA((2 * n + 4 * (3 + many + len(groups)),))]),
        out_shape=[jax.ShapeDtypeStruct(*s) for s in shapes] + [TOKEN],
        compiler_params=_params(),
        cost_estimate=_cost(n * HALF * d * full),
        name="by_states",
    )(me, dep, dq, dkv, *weights, *(a for _, a, _ in adds))


def _block(me, r):
    bits = [(4, lax.div(me, 4)), (2, lax.rem(lax.div(me, 2), 2)), (1, lax.rem(me, 2))]
    return sum(n * ((1 - bit) if r & n else bit) for n, bit in bits)


def _exchange(dep, dq, dkv, wq, wk, wv, *refs, give, keep, plain):
    n, late, some = len(keep), len(give) > len(keep), len(plain) > 0
    kept, late_hbm, plain_hbm, tok = refs[:n], refs[n], refs[n + some], refs[n + late + some]
    lhs_s, w_s, give_s, got_s, sum_s, out_s, sem, send_sem, recv_sem = refs[n + late + some + 1 :]
    tok[...] = jnp.zeros_like(tok)
    me = lax.axis_index("tp")
    other = {"tp": _block(me, 1)}
    d, cols, mine = w_s.shape[0], dq.shape[1], n * HALF
    copies, parts, rows = _Copies(sem), _parts(d, (0, 1, 3, 5, 6, 7)), _rows(len(give) + len(plain) + n)
    given, out = len(give) * HALF, (len(give) + len(plain)) * HALF
    loads = []
    for (r, i), row in zip(give + plain + keep, rows):
        there = pl.ds(pl.multiple_of((_block(me, r) * 2 + i) * HALF, HALF), HALF)
        loads += copies.start([(dq.at[there, :], lhs_s.at[row, :cols]), (dkv.at[there, :], lhs_s.at[row, cols:])])
    loads = [(loads if c == 0 else []) + copies.start(_stacked((wq, wk, wv), w_s, part)) for c, part in enumerate(parts)]
    barrier = pltpu.get_barrier_semaphore()
    pl.semaphore_signal(barrier, inc=1, device_id=other, device_id_type=pl.DeviceIdType.MESH)
    pl.semaphore_wait(barrier, 1)

    def crossing(c):
        pairs = [(give_s.at[:mine, parts[c]], got_s.at[:, parts[c]])]
        if late:
            pairs.append((give_s.at[mine:given, parts[c]], late_hbm.at[:, parts[c]]))
        at = [c * len(pairs) + i for i in range(len(pairs))]
        return [pltpu.make_async_remote_copy(src_ref=a, dst_ref=b, send_sem=send_sem.at[m], recv_sem=recv_sem.at[m], device_id=other,
                                             device_id_type=pl.DeviceIdType.MESH) for m, (a, b) in zip(at, pairs)]

    def add(c):
        for x in sent[c]:
            x.wait_recv()
        wide = parts[c].size
        out_s[:, parts[c]] = (sum_s[c % 2, :, :wide] + got_s[:, parts[c]].astype(F32)).astype(BF16)
        return copies.start([(out_s.at[rows[i], parts[c]], kept[i].at[:, parts[c]]) for i in range(n)])

    sent, stores = [], []
    for c, part in enumerate(parts):
        _wait(loads[c])
        got = _dot(lhs_s[...], w_s[part, :], 1, 1)
        give_s[:, part] = got[:out].astype(BF16)
        sum_s[c % 2, :, : part.size] = got[out:]
        if c:
            stores += add(c - 1)
        sent.append(crossing(c))
        for x in sent[c]:
            x.start()
        if some:
            stores += copies.start([(give_s.at[given:, part], plain_hbm.at[:, part])])
    stores += add(len(parts) - 1)
    _wait(stores)
    for x in sum(sent, []):
        x.wait_send()


def exchange(dep, give, keep, plain, dq, dkv, weights, collective_id):
    d, n, full = weights[0].shape[0], len(keep), sum(w.shape[1] for w in weights)
    more, parts = len(give) - n, 5
    outs = [jax.ShapeDtypeStruct((HALF, d), BF16)] * n + [jax.ShapeDtypeStruct((m * HALF, d), BF16) for m in (more, len(plain)) if m]
    total = len(give) + len(plain) + n
    return pl.pallas_call(
        functools.partial(_exchange, give=give, keep=keep, plain=plain),
        in_specs=[ANY] * 6, out_specs=[ANY] * len(outs) + [pl.BlockSpec(memory_space=pltpu.VMEM)],
        scratch_shapes=[pltpu.VMEM((total * HALF, full), BF16), pltpu.VMEM((d, full), BF16), pltpu.VMEM(((total - n) * HALF, d), BF16),
                        pltpu.VMEM((n * HALF, d), BF16), pltpu.VMEM((2, n * HALF, 2 * d // 7), F32), pltpu.VMEM((n * HALF, d), BF16),
                        pltpu.SemaphoreType.DMA((2 * total + parts * (4 + n),)), pltpu.SemaphoreType.DMA((2 * parts,)), pltpu.SemaphoreType.DMA((2 * parts,))],
        out_shape=outs + [TOKEN],
        compiler_params=pltpu.CompilerParams(vmem_limit_bytes=VMEM, collective_id=collective_id, has_side_effects=True),
        cost_estimate=_cost(total * HALF * d * full),
        name="exchange",
    )(dep, dq, dkv, *weights)


def _by_qkv(me, dep, a, dqt, dkvt, *refs, extra):
    gq, gk, gv, tok, r_s = refs[extra:]
    tok[...] = jnp.zeros_like(tok)
    wide = dqt.shape[0]
    r_s[:wide] = _dot(dqt[...], a[...], 1, 0)
    r_s[wide:] = _dot(dkvt[...], a[...], 1, 0)
    for h in range(r_s.shape[0] // HEAD):
        t = r_s[h * HEAD : (h + 1) * HEAD].T.astype(BF16)
        if h * HEAD < wide:
            gq[:, h * HEAD : (h + 1) * HEAD] = t
        else:
            (gk if h * HEAD == wide else gv)[...] = t


def by_qkv(dep, me, a, dqt, dkvt, lo, hi, before, bm=1024):
    (rows, d), width, extra = a.shape, dqt.shape[0], len(before)
    return pl.pallas_call(
        functools.partial(_by_qkv, extra=extra),
        grid_spec=pltpu.PrefetchScalarGridSpec(
            num_scalar_prefetch=1, grid=(hi - lo,),
            in_specs=[ANY, pl.BlockSpec((rows, bm), lambda j, _: (0, lo + j)), _whole(*dqt.shape), _whole(*dkvt.shape)] + [ANY] * extra,
            out_specs=[pl.BlockSpec((bm, w), lambda j, _: (lo + j, 0)) for w in (width, HEAD, HEAD)] + [TOKEN_SPEC],
            scratch_shapes=[pltpu.VMEM((width + 2 * HEAD, bm), F32)]),
        out_shape=[jax.ShapeDtypeStruct((d, w), BF16) for w in (width, HEAD, HEAD)] + [TOKEN],
        input_output_aliases={5 + i: i for i in range(extra)},
        compiler_params=_params(),
        cost_estimate=_cost(rows * (hi - lo) * bm * (width + 2 * HEAD)),
        name="by_qkv",
    )(me, dep, a, dqt, dkvt, *before)


def _by_wo(me, dep, g, seen_t, out, tok):
    tok[...] = jnp.zeros_like(tok)
    out[...] = _dot(seen_t[...], g[...], 1, 0).astype(BF16)


def by_wo(dep, me, g, seen_t, bn=1024):
    (rows, d), width = g.shape, seen_t.shape[0]
    return pl.pallas_call(
        _by_wo,
        grid_spec=pltpu.PrefetchScalarGridSpec(
            num_scalar_prefetch=1, grid=(d // bn,), in_specs=[ANY, pl.BlockSpec((rows, bn), lambda j, _: (0, j)), _whole(width, rows)],
            out_specs=[pl.BlockSpec((width, bn), lambda j, _: (0, j)), TOKEN_SPEC]),
        out_shape=[jax.ShapeDtypeStruct((width, d), BF16), TOKEN],
        compiler_params=_params(),
        cost_estimate=_cost(rows * d * width),
        name="by_wo",
    )(me, dep, g, seen_t)


def _finish(dep, own, r40, r41, r20, r21, x, dy, gain, by_x, by_gain, own_s, far_s, near_s, x_s, dy_s, out_s, sum_s, sem, out_sem, *, block, wide):
    _, d = own_s.shape
    steps, columns = HALF // block, [pl.ds(c, wide) for c in range(0, d, wide)]

    def copies(half, c):
        mine, here = pl.ds(c * block, block), pl.ds(half * HALF + c * block, block)
        pairs = [(x.at[here, :], x_s), (own.at[here, :], own_s), ((r40, r41)[half].at[mine, :], far_s), ((r20, r21)[half].at[mine, :], near_s), (dy.at[here, :], dy_s)]
        at = (half * steps + c) * len(pairs)
        return here, [pltpu.make_async_copy(a, b.at[here, :], sem.at[at + i]) for i, (a, b) in enumerate(pairs)]

    def result(half, c):
        here = pl.ds(half * HALF + c * block, block)
        return pltpu.make_async_copy(out_s.at[here, :], by_x.at[here, :], out_sem.at[half * steps + c])

    for half in (0, 1):
        for c in range(steps):
            for copy in copies(half, c)[1]:
                copy.start()
    sum_s[...] = jnp.zeros_like(sum_s)
    for half in (0, 1):
        def chunk(c, _):
            here, landed = copies(half, c)
            _wait(landed)
            total = jnp.zeros((block, wide), F32)
            for col in columns:
                total += x_s[here, col].astype(F32) ** 2
            scale = lax.rsqrt(jnp.sum(total, -1, keepdims=True) / d + 1e-6)
            total = jnp.zeros((block, wide), F32)
            for col in columns:
                da = own_s[here, col] + far_s[here, col].astype(F32) + near_s[here, col].astype(F32)
                own_s[here, col] = da
                both = da * (x_s[here, col].astype(F32) * scale)
                sum_s[:, col] += both
                total += both * gain[:, col].astype(F32)
            mean = jnp.sum(total, -1, keepdims=True) / d * scale
            for col in columns:
                inner = own_s[here, col] * gain[:, col].astype(F32) - x_s[here, col].astype(F32) * mean
                out_s[here, col] = (dy_s[here, col].astype(F32) + scale * inner).astype(BF16)
            result(half, c).start()

        lax.fori_loop(0, steps, chunk, None)
    by_gain[...] = jnp.sum(sum_s[...], 0, keepdims=True)
    for half in (0, 1):
        for c in range(steps):
            result(half, c).wait()


def finish(dep, own, sent, x, dy, gain, block=16):
    rows, d = x.shape
    vmem = pl.BlockSpec(memory_space=pltpu.VMEM)
    return pl.pallas_call(
        functools.partial(_finish, block=block, wide=d // 7),
        in_specs=[ANY] * 8 + [vmem], out_specs=[ANY, vmem],
        scratch_shapes=[pltpu.VMEM((rows, d), F32)] + [pltpu.VMEM((rows, d), BF16)] * 5
        + [pltpu.VMEM((block, d), F32), pltpu.SemaphoreType.DMA((5 * rows // block,)), pltpu.SemaphoreType.DMA((rows // block,))],
        out_shape=[jax.ShapeDtypeStruct((rows, d), BF16), jax.ShapeDtypeStruct((1, d), F32)],
        compiler_params=pltpu.CompilerParams(vmem_limit_bytes=VMEM),
        cost_estimate=_cost(rows * d * HEAD),
        name="finish",
    )(dep, own, *sent, x, dy, gain.reshape(1, d))


def _add_up(part, total, all_s, sem, send_sem, recv_sem):
    me = lax.axis_index("tp")
    others = [_block(me, r) for r in range(1, 8)]
    barrier = pltpu.get_barrier_semaphore()
    for other in others:
        pl.semaphore_signal(barrier, inc=1, device_id={"tp": other}, device_id_type=pl.DeviceIdType.MESH)
    mine = pltpu.make_async_copy(part, all_s.at[me], sem)
    mine.start()
    pl.semaphore_wait(barrier, len(others))
    sends = [pltpu.make_async_remote_copy(src_ref=part, dst_ref=all_s.at[me], send_sem=send_sem.at[i], recv_sem=recv_sem.at[me],
                                          device_id={"tp": other}, device_id_type=pl.DeviceIdType.MESH) for i, other in enumerate(others)]
    for copy in sends:
        copy.start()
    mine.wait()
    for other in others:
        pltpu.make_async_copy(part, all_s.at[other], recv_sem.at[other]).wait()
    total[...] = sum(all_s[i] for i in range(1, 8)) + all_s[0]
    for copy in sends:
        copy.wait_send()


def add_up(part):
    dma = pltpu.SemaphoreType.DMA
    return pl.pallas_call(
        _add_up, in_specs=[ANY], out_specs=pl.BlockSpec(memory_space=pltpu.VMEM),
        scratch_shapes=[pltpu.VMEM((8, *part.shape), F32), dma, dma((7,)), dma((8,))],
        out_shape=jax.ShapeDtypeStruct(part.shape, F32),
        compiler_params=pltpu.CompilerParams(collective_id=2, has_side_effects=True),
        name="add_up",
    )(part)


def swap(value, r):
    return lax.ppermute(value, "tp", [(i, i ^ r) for i in range(8)])


def normed(x, gain):
    wide = x.astype(F32)
    scale = lax.rsqrt(jnp.mean(wide * wide, -1, keepdims=True) + 1e-6)
    return (wide * scale * gain.astype(F32)).astype(BF16)


def gather(halves):
    got = {(0, i): t for i, t in enumerate(halves)}

    def send(r, i, by):
        got[r, i] = swap(got[r ^ by, i], by)

    for r, i in ((4, 0), (2, 1), (1, 0), (1, 1), (4, 1), (2, 0)):
        send(r, i, r)
    send(6, 0, 2)
    send(6, 1, 4)
    for r, i in ((4, 0), (2, 1), (4, 1), (2, 0), (6, 0), (6, 1)):
        send(r ^ 1, i, 1)
    return got


def solution(mesh):
    def step(x, dy, gain, wq, wk, wv, wo):
        me = lax.axis_index("tp").astype(jnp.int32).reshape(1)
        rows, weights = x.shape[0] * 8, [wq, wk, wv]
        angle = jnp.arange(rows).astype(F32)[:, None] * THETA ** (-jnp.arange(HEAD // 2, dtype=F32) / (HEAD // 2))
        cos, sin = jnp.cos(angle), jnp.sin(angle)
        cos_w, sin_w = jnp.concatenate([cos, cos], 1), jnp.concatenate([-sin, sin], 1)
        cos_t, sin_t = cos.T, sin.T
        both = lambda r: [(r, 0), (r, 1)]
        order = [both(0) + both(1), [(4, 0), (5, 0), (2, 1), (3, 1)], [(4, 1), (5, 1), (2, 0), (3, 0)], both(6) + both(7)]

        a = gather([normed(x[:HALF], gain), normed(x[HALF:], gain)])

        def projected(n, token, before, through=()):
            return project(token, me, [a[key] for key in order[n]], order[n], weights, cos_w, sin_w, before, through)

        def seen_grad(n, token, before):
            return by_seen(token, me, [g[key] for key in order[n]], order[n], wo, rows, before)

        *known, token = projected(0, jnp.zeros(TOKEN.shape, F32), [])
        *known, g0, g1, token = projected(1, token, known, [dy[:HALF], dy[HALF:]])
        g = gather([g0, g1])
        *known, token = projected(2, token, known)
        *grads, token = seen_grad(0, token, [])
        *known, token = projected(3, token, known)
        q, k, v, states = known
        out, lse, token = attend(token, me, q, k, v)
        heads = q.shape[0]

        def attention_back(rs, token, before, last):
            return back(token, me, rs, q, k, v, grads[0].reshape(heads, HEAD, rows), out, lse, cos_t, sin_t, before, last)

        *sums, token = attention_back((0,), token, None, False)
        *grads, token = seen_grad(1, token, grads)
        *grads, token = seen_grad(2, token, grads)
        *sums, token = attention_back((4, 2), token, sums, False)
        *grads, token = seen_grad(3, token, grads)
        dq, dq_t, dkv, dkv_t, token = attention_back((6,), token, sums, True)

        def term(token, keys, groups, adds=(), dtypes=(BF16,) * 4):
            return by_states(token, me, keys, dq, dkv, weights, adds, groups, dtypes)

        s60, s61, token = exchange(token, both(7), both(6), [], dq, dkv, weights, 0)
        far2, far4 = swap(s60, 4), swap(s61, 2)
        s40, s21, got, t1, token = exchange(token, [(5, 0), (3, 1), (5, 1), (3, 0)], [(4, 0), (2, 1)], both(1), dq, dkv, weights, 1)
        r40, r21 = swap(s40, 4), swap(s21, 2)
        p0 = swap(t1, 1)
        by_o, token = by_wo(token, me, grads[1], out.reshape(heads * HEAD, rows))
        s41, s20, own, token = term(token, [(4, 1), (2, 0)] + both(0), [1, 1, 2],
                                    [(0, got, 0), (0, far4, 0), (1, got, 1), (1, far2, 0), (2, p0, 0), (3, p0, 1)], (BF16, BF16, F32))
        r41, r20 = swap(s41, 4), swap(s20, 2)
        *by_w, token = by_qkv(token, me, states, dq_t, dkv_t, 0, 7, [])
        by_x, by_gain = finish(token, own, [r40, r41, r20, r21], x, dy, gain)
        return (by_x, add_up(by_gain), *by_w, by_o)

    tokens, columns = P(("dp", "tp"), None), P(None, "tp")
    return jax.shard_map(
        step,
        mesh=mesh,
        in_specs=(tokens, tokens, P(None), columns, columns, columns, P("tp", None)),
        out_specs=(tokens, P("dp", None), P("dp", "tp"), P("dp", "tp"), P("dp", "tp"), P(("dp", "tp"), None)),
        check_vma=False,
    )
```

```python
import functools

import jax
import jax.numpy as jnp
from jax import lax
from jax.experimental import pallas as pl
from jax.experimental.pallas import tpu as pltpu
from jax.sharding import PartitionSpec as P


HEAD = 128
THETA = 10000
NEG = -1e30
HIDDEN = 2 * NEG
LOG2E = 1.4426950408889634
VMEM = 67043328
F32, BF16 = jnp.float32, jnp.bfloat16
ANY = pl.BlockSpec(memory_space=pltpu.HBM)
IN_VMEM = pl.BlockSpec(memory_space=pltpu.VMEM)
TOKEN = jax.ShapeDtypeStruct((8, 128), F32)
TOKEN_SPEC = pl.BlockSpec(TOKEN.shape, lambda i, _: (0, 0))


def _dot(a, b, ca, cb):
    return lax.dot_general(a, b, (((ca,), (cb,)), ((), ())), preferred_element_type=F32)


def _params():
    return pltpu.CompilerParams(dimension_semantics=("arbitrary",), vmem_limit_bytes=VMEM)


def _meeting(collective_id):
    return pltpu.CompilerParams(vmem_limit_bytes=VMEM, collective_id=collective_id, has_side_effects=True)


def _sems(n):
    return pltpu.SemaphoreType.DMA((n,))


def _cost(products):
    return pl.CostEstimate(flops=2 * products, bytes_accessed=products // 64, transcendentals=0)


def _whole(*shape):
    return pl.BlockSpec(shape, lambda i, _: (0, 0))


HALF = 128


def _block(me, r):
    bits = [(4, lax.div(me, 4)), (2, lax.rem(lax.div(me, 2), 2)), (1, lax.rem(me, 2))]
    return sum(n * ((1 - bit) if r & n else bit) for n, bit in bits)


def _at(me, key):
    return pl.multiple_of((_block(me, key[0]) * 2 + key[1]) * HALF, HALF)


def _rows(n):
    return [pl.ds(i * HALF, HALF) for i in range(n)]


def _parts(size, cuts=(0, 1, 3, 5, 7)):
    return [pl.ds(lo * size // 7, (hi - lo) * size // 7) for lo, hi in zip(cuts, cuts[1:])]


def _pairs(keys):
    return keys + [(r ^ 1, i) for r, i in keys]


class _Copies:
    def __init__(self, sem):
        self.sem, self.used = sem, 0

    def start(self, pairs):
        made = []
        for src, dst in pairs:
            made.append(pltpu.make_async_copy(src, dst, self.sem.at[self.used]))
            made[-1].start()
            self.used += 1
        return made


class _Stream:
    def __init__(self, copies, parts, pairs):
        self.copies, self.parts, self.pairs, self.made = copies, parts, pairs, []
        self.more()

    def more(self):
        if len(self.made) < len(self.parts):
            self.made.append(self.copies.start(self.pairs(self.parts[len(self.made)])))

    def take(self, c):
        if c == 0:
            self.more()
        _wait(self.made[c])
        self.more()


def _greet(others):
    barrier = pltpu.get_barrier_semaphore()
    for other in others:
        pl.semaphore_signal(barrier, inc=1, device_id={"tp": other}, device_id_type=pl.DeviceIdType.MESH)
    pl.semaphore_wait(barrier, len(others))


def _remote(src, dst, send_sem, recv_sem, other):
    return pltpu.make_async_remote_copy(src_ref=src, dst_ref=dst, send_sem=send_sem, recv_sem=recv_sem, device_id={"tp": other},
                                        device_id_type=pl.DeviceIdType.MESH)


def _crossing(pieces, target, parts, rows, send_sem, recv_sem):
    other, n = _block(lax.axis_index("tp"), 1), len(pieces)
    _greet([other])
    made = [[_remote(p.at[:, part], target.at[r, part], send_sem.at[c * n + i], recv_sem.at[c * n + i], other) for i, (p, r) in enumerate(zip(pieces, rows))]
            for c, part in enumerate(parts)]
    for x in sum(made, []):
        x.start()
    return made


def _wait(copies):
    for c in copies:
        c.wait()


def _stacked(weights, w_s, part):
    at, pairs = 0, []
    for w in weights:
        pairs.append((w.at[part, :], w_s.at[part, at : at + w.shape[1]]))
        at += w.shape[1]
    return pairs


def _project(dep, *refs, keys, heads, extra, through):
    n, me = len(keys), lax.axis_index("tp")
    pieces, (wq, wk, wv, cos, sin), refs = refs[:n], refs[n : n + 5], refs[n + 5 + extra :]
    q_hbm, k_hbm, v_hbm, a_hbm = refs[:4]
    tok, a_s, w_s, cos_s, sin_s, acc, q_s, k_s, v_s, sem, send_sem, recv_sem = refs[4 + through :]
    tok[...] = jnp.zeros_like(tok)
    rows, tokens = _rows(2 * n), [pl.ds(_at(me, key), HALF) for key in _pairs(keys)]
    copies, parts = _Copies(sem), _parts(a_s.shape[1])
    loads = _Stream(copies, parts, lambda part: [(p.at[:, part], a_s.at[r, part]) for p, r in zip(pieces, rows)] + _stacked((wq, wk, wv), w_s, part))
    tables = copies.start([(t.at[there, :], s.at[r, :]) for t, s in ((cos, cos_s), (sin, sin_s)) for r, there in zip(rows, tokens)])
    crossing = _crossing(pieces, a_s, parts, rows[n:], send_sem, recv_sem)
    for c, part in enumerate(parts):
        loads.take(c)
        for x in crossing[c]:
            x.wait_recv()
        if part is parts[-1]:
            stores = copies.start([(a_s.at[r, :], a_hbm.at[there, :]) for r, there in zip(rows, tokens)])
        got = _dot(a_s[:, part], w_s[part, :], 1, 0)
        acc[...] = got if c == 0 else acc[...] + got
    _wait(tables)
    for h in range(heads + 2):
        t = acc[:, h * HEAD : (h + 1) * HEAD].astype(BF16)
        if h <= heads:
            t = t.astype(F32)
            t = (t * cos_s[...] + pltpu.roll(t, HEAD // 2, 1) * sin_s[...]).astype(BF16)
        if h < heads:
            q_s[h] = t
        else:
            (k_s if h == heads else v_s)[...] = t
    for r, there in zip(rows, tokens):
        stores += copies.start([(q_s.at[:, r, :], q_hbm.at[:, there, :]), (k_s.at[r, :], k_hbm.at[there, :]), (v_s.at[r, :], v_hbm.at[there, :])])
    _wait(stores)
    for x in sum(crossing, []):
        x.wait_send()


def project(dep, collective_id, pieces, keys, weights, cos, sin, before, through=()):
    (d, width), more = weights[0].shape, weights[1].shape[1]
    heads, rows, n, full = width // HEAD, cos.shape[0], len(pieces), width + 2 * more
    total, extra = 2 * n * HALF, len(before) + len(through)
    outs = [jax.ShapeDtypeStruct(s, BF16) for s in ((heads, rows, HEAD), (rows, HEAD), (rows, HEAD), (rows, d))]
    outs += [jax.ShapeDtypeStruct(t.shape, t.dtype) for t in through]
    first = 1 + n + 5
    return pl.pallas_call(
        functools.partial(_project, keys=keys, heads=heads, extra=extra, through=len(through)),
        in_specs=[ANY] * (first + extra), out_specs=[ANY] * len(outs) + [IN_VMEM],
        scratch_shapes=[pltpu.VMEM((total, d), BF16), pltpu.VMEM((d, full), BF16), pltpu.VMEM((total, HEAD), F32), pltpu.VMEM((total, HEAD), F32),
                            pltpu.VMEM((total, full), F32), pltpu.VMEM((heads, total, HEAD), BF16), pltpu.VMEM((total, HEAD), BF16),
                            pltpu.VMEM((total, HEAD), BF16), _sems(20 * n + 12), _sems(4 * n), _sems(4 * n)],
        out_shape=outs + [TOKEN],
        input_output_aliases={first + i: len(outs) - extra + i for i in range(extra)},
        compiler_params=_meeting(collective_id),
        cost_estimate=_cost(total * d * full),
        name="project",
    )(dep, *pieces, *weights, cos, sin, *before, *through)


def _by_seen(dep, *refs, keys, extra):
    n, me = len(keys), lax.axis_index("tp")
    pieces, wo, (out_hbm, g_hbm, tok, g_s, w_s, acc, stage, sem, send_sem, recv_sem) = refs[:n], refs[n], refs[n + 1 + extra :]
    tok[...] = jnp.zeros_like(tok)
    rows, tokens = _rows(2 * n), [pl.ds(_at(me, key), HALF) for key in _pairs(keys)]
    copies, parts = _Copies(sem), _parts(g_s.shape[1])
    loads = _Stream(copies, parts, lambda part: [(p.at[:, part], g_s.at[r, part]) for p, r in zip(pieces, rows)] + [(wo.at[:, part], w_s.at[:, part])])
    crossing = _crossing(pieces, g_s, parts, rows[n:], send_sem, recv_sem)
    for c, part in enumerate(parts):
        loads.take(c)
        for x in crossing[c]:
            x.wait_recv()
        if part is parts[-1]:
            stores = copies.start([(g_s.at[r, :], g_hbm.at[there, :]) for r, there in zip(rows, tokens)])
        got = _dot(w_s[:, part], g_s[:, part], 1, 1)
        acc[...] = got if c == 0 else acc[...] + got
    stage[...] = acc[...].astype(BF16)
    _wait(stores + copies.start([(stage.at[:, r], out_hbm.at[:, there]) for r, there in zip(rows, tokens)]))
    for x in sum(crossing, []):
        x.wait_send()


def by_seen(dep, collective_id, pieces, keys, wo, rows, before):
    width, d = wo.shape
    n, extra = len(pieces), len(before)
    total = 2 * n * HALF
    return pl.pallas_call(
        functools.partial(_by_seen, keys=keys, extra=extra),
        in_specs=[ANY] * (n + 2 + extra), out_specs=[ANY, ANY, IN_VMEM],
        scratch_shapes=[pltpu.VMEM((total, d), BF16), pltpu.VMEM((width, d), BF16), pltpu.VMEM((width, total), F32), pltpu.VMEM((width, total), BF16),
                            _sems(12 * n + 4), _sems(4 * n), _sems(4 * n)],
        out_shape=[jax.ShapeDtypeStruct((width, rows), BF16), jax.ShapeDtypeStruct((rows, d), BF16), TOKEN],
        input_output_aliases={2 + n + i: i for i in range(extra)},
        compiler_params=_meeting(collective_id),
        cost_estimate=_cost(total * d * width),
        name="by_seen",
    )(dep, *pieces, wo, *before)


def _attend(me, dep, q_ref, k_ref, v_ref, o_ref, lse_ref, tok, top_s, mix_s, gap_s, *, scale, bq):
    g, d = q_ref.shape[0], q_ref.shape[2]
    iq = pl.program_id(0)
    e = scale * LOG2E

    @pl.when(iq == 0)
    def _():
        tok[...] = jnp.zeros_like(tok)
        gap_s[...] = lax.broadcasted_iota(jnp.int32, gap_s.shape, 1) - lax.broadcasted_iota(jnp.int32, gap_s.shape, 0)

    top_s[...] = jnp.full_like(top_s, NEG)
    mix_s[...] = jnp.zeros_like(mix_s)

    def block(first, keys, lo, masked):
        here, there = pl.ds(pl.multiple_of(first, keys), keys), pl.ds(lo, bq - lo)
        scores = [_dot(k_ref[here, :], q_ref[n, there, :], 1, 1) for n in range(g)]
        weights, keeps = [], []
        for n, s in enumerate(scores):
            if masked:
                s = jnp.where(gap_s[:keys, : bq - lo] >= 0, s, HIDDEN)
            old = top_s[n : n + 1, there]
            top = jnp.maximum(old, s.max(axis=0, keepdims=True))
            top_s[n : n + 1, there] = top
            weights.append(jnp.exp2((s - top) * e).astype(BF16))
            keeps.append(jnp.exp2((old - top) * e))
        values = jnp.concatenate([v_ref[here, :].T, jnp.ones((8, keys), BF16)], axis=0)
        for n, (p, keep) in enumerate(zip(weights, keeps)):
            mix_s[n, :, there] = mix_s[n, :, there] * keep + _dot(values, p, 1, 0)

    lax.fori_loop(0, iq, lambda j, _: block(j * bq, bq, 0, False), None)
    for lo in (0, bq // 2):
        block(iq * bq + lo, bq // 2, lo, True)
    for n in range(g):
        total = mix_s[n, d : d + 1, :]
        o_ref[n] = (mix_s[n, :d, :] * (1 / total)).astype(BF16)
        lse_ref[n : n + 1, :] = top_s[n : n + 1, :] * scale + jnp.log(total)


def attend(dep, me, q, k, v, bq=512):
    g, rows, d = q.shape
    whole = _whole(rows, d)
    return pl.pallas_call(
        functools.partial(_attend, scale=d**-0.5, bq=bq),
        grid_spec=pltpu.PrefetchScalarGridSpec(
            num_scalar_prefetch=1, grid=(rows // bq,),
            in_specs=[ANY, pl.BlockSpec((g, bq, d), lambda i, _: (0, i, 0)), whole, whole],
            out_specs=[pl.BlockSpec((g, d, bq), lambda i, _: (0, 0, i)), pl.BlockSpec((g, bq), lambda i, _: (0, i)),
                       TOKEN_SPEC],
            scratch_shapes=[pltpu.VMEM((g, bq), F32), pltpu.VMEM((g, d + 8, bq), F32), pltpu.VMEM((bq // 2, bq), jnp.int32)]),
        out_shape=[jax.ShapeDtypeStruct((g, d, rows), BF16), jax.ShapeDtypeStruct((g, rows), F32), TOKEN],
        compiler_params=_params(),
        cost_estimate=_cost(2 * g * rows * rows * d),
        name="attend",
    )(me, dep, q, k, v)


def _chip(me, i, rs):
    r = rs[0]
    for n in range(1, len(rs)):
        r = jnp.where(i == n, rs[n], r)
    return (me[0] ^ r) // 2


def _back(me, dep, q_ref, k_ref, v_ref, do_ref, o_ref, lse_ref, cos, sin, *refs, scale, bq, first, last, rs):
    g, d = q_ref.shape[0], q_ref.shape[2]
    if not first:
        dk_in, dv_in, refs = refs[0], refs[1], refs[2 + (2):]
    if last:
        dq_ref, dqt_ref, dkv_ref, dkvt_ref, tok, dq_s, gap_s, dk_s, dv_s = refs
    else:
        dq_ref, dqt_ref, dk_s, dv_s, tok, dq_s, gap_s = refs
    i = pl.program_id(0)
    iq = _chip(me, i, rs)
    e = scale * LOG2E
    half = d // 2

    @pl.when(i == 0)
    def _():
        tok[...] = jnp.zeros_like(tok)
        gap_s[...] = lax.broadcasted_iota(jnp.int32, gap_s.shape, 1) - lax.broadcasted_iota(jnp.int32, gap_s.shape, 0)
        if first:
            dk_s[...] = jnp.zeros_like(dk_s)
            dv_s[...] = jnp.zeros_like(dv_s)
        else:
            dk_s[...] = dk_in[...]
            dv_s[...] = dv_in[...]

    dq_s[...] = jnp.zeros_like(dq_s)
    lses = [lse_ref[n : n + 1, :] * LOG2E for n in range(g)]
    deltas = [(do_ref[n].astype(F32) * o_ref[n].astype(F32)).sum(0, keepdims=True) for n in range(g)]

    def block(first, keys, lo, masked):
        here, there = pl.ds(pl.multiple_of(first, keys), keys), pl.ds(lo, bq - lo)
        scores = [_dot(k_ref[here, :], q_ref[n, there, :], 1, 1) for n in range(g)]
        dps = [_dot(v_ref[here, :], do_ref[n, :, there], 1, 0) for n in range(g)]
        kt = k_ref[here, :].T
        for n in range(g):
            p = jnp.exp2(scores[n] * e - lses[n][:, lo:])
            if masked:
                p = jnp.where(gap_s[:keys, : bq - lo] >= 0, p, 0.0)
            ds = (p * (dps[n] - deltas[n][:, lo:])).astype(BF16)
            dv_s[here, :] += _dot(p.astype(BF16), do_ref[n, :, there], 1, 1)
            dk_s[here, :] += _dot(ds, q_ref[n, there, :], 1, 0)
            dq_s[n, :, there] += _dot(kt, ds, 1, 0)

    lax.fori_loop(0, iq, lambda j, _: block(j * bq, bq, 0, False), None)
    for lo in (0, bq // 2):
        block(iq * bq + lo, bq // 2, lo, True)

    def unturned(t, c, s):
        t = t.astype(BF16).astype(F32)
        a, b = t[:half], t[half:]
        return jnp.concatenate([a * c + b * s, b * c - a * s], axis=0)

    at = pl.ds(pl.multiple_of(iq * bq, bq), bq)
    for n in range(g):
        t = unturned(dq_s[n] * scale, cos[:, at], sin[:, at])
        dqt_ref[n * d : (n + 1) * d, :] = t.astype(BF16)
        dq_ref[:, n * d : (n + 1) * d] = t.T.astype(BF16)

    if last:
        @pl.when(i == len(rs) - 1)
        def _():
            t = unturned((dk_s[...] * scale).T, cos[...], sin[...])
            dkvt_ref[:d, :] = t.astype(BF16)
            dkv_ref[:, :d] = t.T.astype(BF16)
            dkvt_ref[d:, :] = dv_s[...].T.astype(BF16)
            dkv_ref[:, d:] = dv_s[...].astype(BF16)


def back(dep, me, rs, q, k, v, do_t, out_t, lse, cos_t, sin_t, before, last):
    g, rows, d = q.shape
    first, bq = before is None, rows // 4
    here = lambda i, me: _chip(me, i, rs)
    whole = _whole(rows, d)
    table = _whole(d // 2, rows)
    across = pl.BlockSpec((g, d, bq), lambda i, me: (0, 0, here(i, me)))
    specs = [ANY, pl.BlockSpec((g, bq, d), lambda i, me: (0, here(i, me), 0)), whole, whole, across, across, pl.BlockSpec((g, bq), lambda i, me: (0, here(i, me))), table, table]
    given = [dep, q, k, v, do_t, out_t, lse, cos_t, sin_t]
    aliases = {}
    if not first:
        specs += [whole, whole, ANY, ANY]
        given += [before[2], before[3], before[0], before[1]]
        aliases = {2 + 10: 0, 2 + 11: 1}
    outs = [jax.ShapeDtypeStruct((rows, g * d), BF16), jax.ShapeDtypeStruct((g * d, rows), BF16)]
    out_specs = [pl.BlockSpec((bq, g * d), lambda i, me: (here(i, me), 0)), pl.BlockSpec((g * d, bq), lambda i, me: (0, here(i, me)))]
    scratch = [pltpu.VMEM((g, d, bq), F32), pltpu.VMEM((bq // 2, bq), jnp.int32)]
    if last:
        outs += [jax.ShapeDtypeStruct((rows, 2 * d), BF16), jax.ShapeDtypeStruct((2 * d, rows), BF16)]
        out_specs += [_whole(rows, 2 * d), _whole(2 * d, rows)]
        scratch += [pltpu.VMEM((rows, d), F32)] * 2
    else:
        outs += [jax.ShapeDtypeStruct((rows, d), F32)] * 2
        out_specs += [whole, whole]
    return pl.pallas_call(
        functools.partial(_back, scale=d**-0.5, bq=bq, first=first, last=last, rs=rs),
        grid_spec=pltpu.PrefetchScalarGridSpec(num_scalar_prefetch=1, grid=(len(rs),), in_specs=specs,
                                               out_specs=out_specs + [pl.BlockSpec((8, 128), lambda i, b: (0, 0))], scratch_shapes=scratch),
        out_shape=outs + [TOKEN],
        input_output_aliases=aliases,
        compiler_params=_params(),
        cost_estimate=_cost(4 * g * len(rs) * bq * rows * d),
        name="back",
    )(me, *given)


def _by_states(dep, dq, dkv, wq, wk, wv, *refs, keys, adds, groups):
    n, many, me = len(keys), len(groups), lax.axis_index("tp")
    added, outs, tok, refs = refs[: len(adds)], refs[len(adds) : len(adds) + many], refs[len(adds) + many], refs[len(adds) + many + 1 :]
    stages, (lhs_s, w_s, add_s, sem) = refs[:many], refs[many:]
    tok[...] = jnp.zeros_like(tok)
    rows, cols = _rows(n + len(adds)), dq.shape[1]
    copies, parts = _Copies(sem), _parts(w_s.shape[0])
    first = []
    for key, r in zip(keys, rows):
        there = pl.ds(_at(me, key), HALF)
        first += copies.start([(dq.at[there, :], lhs_s.at[r, :cols]), (dkv.at[there, :], lhs_s.at[r, cols:])])
    loads = _Stream(copies, parts, lambda part: _stacked((wq, wk, wv), w_s, part)
                    + [(a.at[_rows(row + 1)[row], part], add_s.at[r, part]) for a, (_, row), r in zip(added, adds, rows)])
    _wait(first)
    place, stores = [(o, r) for o, k in enumerate(groups) for r in _rows(k)], []
    for c, part in enumerate(parts):
        loads.take(c)
        got = _dot(lhs_s[...], w_s[part, :], 1, 1)
        for i, (o, r) in enumerate(place):
            t = got[i * HALF : (i + 1) * HALF]
            for (target, _), mine in zip(adds, rows):
                if target == i:
                    t = t + add_s[mine, part].astype(F32)
            stages[o][r, part] = t.astype(stages[o].dtype)
        stores += copies.start([(stage.at[:, part], out.at[:, part]) for stage, out in zip(stages, outs)])
    _wait(stores)


def by_states(dep, keys, dq, dkv, weights, adds, groups, dtypes):
    d, n, many, full = weights[0].shape[0], len(keys), len(adds), sum(w.shape[1] for w in weights)
    shapes = [((k * HALF, d), t) for k, t in zip(groups, dtypes)]
    return pl.pallas_call(
        functools.partial(_by_states, keys=keys, adds=[(i, row) for i, _, row in adds], groups=groups),
        in_specs=[ANY] * (6 + many), out_specs=[ANY] * len(groups) + [IN_VMEM],
        scratch_shapes=[pltpu.VMEM(*s) for s in shapes] + [pltpu.VMEM((n * HALF, full), BF16), pltpu.VMEM((d, full), BF16),
                                                               pltpu.VMEM((max(many, 1) * HALF, d), BF16),
                                                               _sems(2 * n + 4 * (3 + many + len(groups)))],
        out_shape=[jax.ShapeDtypeStruct(*s) for s in shapes] + [TOKEN],
        compiler_params=pltpu.CompilerParams(vmem_limit_bytes=VMEM),
        cost_estimate=_cost(n * HALF * d * full),
        name="by_states",
    )(dep, dq, dkv, *weights, *(a for _, a, _ in adds))


def _exchange(dep, dq, dkv, wq, wk, wv, *refs, give, keep, plain):
    n, late, some = len(keep), len(give) > len(keep), len(plain) > 0
    kept, late_hbm, plain_hbm, tok = refs[:n], refs[n], refs[n + some], refs[n + late + some]
    lhs_s, w_s, give_s, got_s, sum_s, out_s, sem, send_sem, recv_sem = refs[n + late + some + 1 :]
    tok[...] = jnp.zeros_like(tok)
    me = lax.axis_index("tp")
    other = _block(me, 1)
    d, cols, mine = w_s.shape[0], dq.shape[1], n * HALF
    copies, parts, rows = _Copies(sem), _parts(d, (0, 1, 3, 5, 6, 7)), _rows(len(give) + len(plain) + n)
    given, out = len(give) * HALF, (len(give) + len(plain)) * HALF
    first = []
    for key, row in zip(give + plain + keep, rows):
        there = pl.ds(_at(me, key), HALF)
        first += copies.start([(dq.at[there, :], lhs_s.at[row, :cols]), (dkv.at[there, :], lhs_s.at[row, cols:])])
    loads = _Stream(copies, parts, lambda part: _stacked((wq, wk, wv), w_s, part))
    _greet([other])
    _wait(first)

    def crossing(c):
        pairs = [(give_s.at[:mine, parts[c]], got_s.at[:, parts[c]])]
        if late:
            pairs.append((give_s.at[mine:given, parts[c]], late_hbm.at[:, parts[c]]))
        at = [c * len(pairs) + i for i in range(len(pairs))]
        return [_remote(a, b, send_sem.at[m], recv_sem.at[m], other) for m, (a, b) in zip(at, pairs)]

    def add(c):
        for x in sent[c]:
            x.wait_recv()
        wide = parts[c].size
        out_s[:, parts[c]] = (sum_s[c % 2, :, :wide] + got_s[:, parts[c]].astype(F32)).astype(BF16)
        return copies.start([(out_s.at[rows[i], parts[c]], kept[i].at[:, parts[c]]) for i in range(n)])

    sent, stores = [], []
    for c, part in enumerate(parts):
        loads.take(c)
        for lo in range(0, part.size, 512):
            some_columns = pl.ds(part.start + lo, 512)
            got = _dot(lhs_s[...], w_s[some_columns, :], 1, 1)
            give_s[:, some_columns] = got[:out].astype(BF16)
            sum_s[c % 2, :, lo : lo + 512] = got[out:]
        if c:
            stores += add(c - 1)
        sent.append(crossing(c))
        for x in sent[c]:
            x.start()
        if some:
            stores += copies.start([(give_s.at[given:, part], plain_hbm.at[:, part])])
    stores += add(len(parts) - 1)
    _wait(stores)
    for x in sum(sent, []):
        x.wait_send()


def exchange(dep, give, keep, plain, dq, dkv, weights, collective_id):
    d, n, full = weights[0].shape[0], len(keep), sum(w.shape[1] for w in weights)
    more, parts = len(give) - n, 5
    outs = [jax.ShapeDtypeStruct((HALF, d), BF16)] * n + [jax.ShapeDtypeStruct((m * HALF, d), BF16) for m in (more, len(plain)) if m]
    total = len(give) + len(plain) + n
    return pl.pallas_call(
        functools.partial(_exchange, give=give, keep=keep, plain=plain),
        in_specs=[ANY] * 6, out_specs=[ANY] * len(outs) + [IN_VMEM],
        scratch_shapes=[pltpu.VMEM((total * HALF, full), BF16), pltpu.VMEM((d, full), BF16), pltpu.VMEM(((total - n) * HALF, d), BF16),
                        pltpu.VMEM((n * HALF, d), BF16), pltpu.VMEM((2, n * HALF, 2 * d // 7), F32), pltpu.VMEM((n * HALF, d), BF16),
                        pltpu.SemaphoreType.DMA((2 * total + parts * (4 + n),)), pltpu.SemaphoreType.DMA((2 * parts,)), pltpu.SemaphoreType.DMA((2 * parts,))],
        out_shape=outs + [TOKEN],
        compiler_params=_meeting(collective_id),
        cost_estimate=_cost(total * HALF * d * full),
        name="exchange",
    )(dep, dq, dkv, *weights)


def _by_qkv(me, dep, a, dqt, dkvt, *refs, extra):
    gq, gk, gv, tok, r_s = refs[extra:]
    tok[...] = jnp.zeros_like(tok)
    wide = dqt.shape[0]
    r_s[:wide] = _dot(dqt[...], a[...], 1, 0)
    r_s[wide:] = _dot(dkvt[...], a[...], 1, 0)
    for h in range(r_s.shape[0] // HEAD):
        t = r_s[h * HEAD : (h + 1) * HEAD].T.astype(BF16)
        if h * HEAD < wide:
            gq[:, h * HEAD : (h + 1) * HEAD] = t
        else:
            (gk if h * HEAD == wide else gv)[...] = t


def by_qkv(dep, me, a, dqt, dkvt, lo, hi, before, bm=1024):
    (rows, d), width, extra = a.shape, dqt.shape[0], len(before)
    return pl.pallas_call(
        functools.partial(_by_qkv, extra=extra),
        grid_spec=pltpu.PrefetchScalarGridSpec(
            num_scalar_prefetch=1, grid=(hi - lo,),
            in_specs=[ANY, pl.BlockSpec((rows, bm), lambda j, _: (0, lo + j)), _whole(*dqt.shape), _whole(*dkvt.shape)] + [ANY] * extra,
            out_specs=[pl.BlockSpec((bm, w), lambda j, _: (lo + j, 0)) for w in (width, HEAD, HEAD)] + [TOKEN_SPEC],
            scratch_shapes=[pltpu.VMEM((width + 2 * HEAD, bm), F32)]),
        out_shape=[jax.ShapeDtypeStruct((d, w), BF16) for w in (width, HEAD, HEAD)] + [TOKEN],
        input_output_aliases={5 + i: i for i in range(extra)},
        compiler_params=_params(),
        cost_estimate=_cost(rows * (hi - lo) * bm * (width + 2 * HEAD)),
        name="by_qkv",
    )(me, dep, a, dqt, dkvt, *before)


def _by_wo(me, dep, g, seen_t, out, tok):
    tok[...] = jnp.zeros_like(tok)
    out[...] = _dot(seen_t[...], g[...], 1, 0).astype(BF16)


def by_wo(dep, me, g, seen_t, bn=1024):
    (rows, d), width = g.shape, seen_t.shape[0]
    return pl.pallas_call(
        _by_wo,
        grid_spec=pltpu.PrefetchScalarGridSpec(
            num_scalar_prefetch=1, grid=(d // bn,), in_specs=[ANY, pl.BlockSpec((rows, bn), lambda j, _: (0, j)), _whole(width, rows)],
            out_specs=[pl.BlockSpec((width, bn), lambda j, _: (0, j)), TOKEN_SPEC]),
        out_shape=[jax.ShapeDtypeStruct((width, d), BF16), TOKEN],
        compiler_params=_params(),
        cost_estimate=_cost(rows * d * width),
        name="by_wo",
    )(me, dep, g, seen_t)


def _finish(dep, own, r40, r41, r20, r21, x, dy, gain, by_x, by_gain, own_s, far_s, near_s, x_s, dy_s, out_s, sum_s, sem, out_sem, *, block, wide):
    _, d = own_s.shape
    steps, columns = HALF // block, [pl.ds(c, wide) for c in range(0, d, wide)]

    def copies(half, c):
        mine, here = pl.ds(c * block, block), pl.ds(half * HALF + c * block, block)
        pairs = [(x.at[here, :], x_s), (own.at[here, :], own_s), ((r40, r41)[half].at[mine, :], far_s), ((r20, r21)[half].at[mine, :], near_s), (dy.at[here, :], dy_s)]
        at = (half * steps + c) * len(pairs)
        return here, [pltpu.make_async_copy(a, b.at[here, :], sem.at[at + i]) for i, (a, b) in enumerate(pairs)]

    def result(half, c):
        here = pl.ds(half * HALF + c * block, block)
        return pltpu.make_async_copy(out_s.at[here, :], by_x.at[here, :], out_sem.at[half * steps + c])

    for half in (0, 1):
        for c in range(steps):
            for copy in copies(half, c)[1]:
                copy.start()
    sum_s[...] = jnp.zeros_like(sum_s)
    for half in (0, 1):
        def chunk(c, _):
            here, landed = copies(half, c)
            _wait(landed)
            total = jnp.zeros((block, wide), F32)
            for col in columns:
                total += x_s[here, col].astype(F32) ** 2
            scale = lax.rsqrt(jnp.sum(total, -1, keepdims=True) / d + 1e-6)
            total = jnp.zeros((block, wide), F32)
            for col in columns:
                da = own_s[here, col] + far_s[here, col].astype(F32) + near_s[here, col].astype(F32)
                own_s[here, col] = da
                both = da * (x_s[here, col].astype(F32) * scale)
                sum_s[:, col] += both
                total += both * gain[:, col].astype(F32)
            mean = jnp.sum(total, -1, keepdims=True) / d * scale
            for col in columns:
                inner = own_s[here, col] * gain[:, col].astype(F32) - x_s[here, col].astype(F32) * mean
                out_s[here, col] = (dy_s[here, col].astype(F32) + scale * inner).astype(BF16)
            result(half, c).start()

        lax.fori_loop(0, steps, chunk, None)
    by_gain[...] = jnp.sum(sum_s[...], 0, keepdims=True)
    for half in (0, 1):
        for c in range(steps):
            result(half, c).wait()


def finish(dep, own, sent, x, dy, gain, block=16):
    rows, d = x.shape
    return pl.pallas_call(
        functools.partial(_finish, block=block, wide=d // 7),
        in_specs=[ANY] * 8 + [IN_VMEM], out_specs=[ANY, IN_VMEM],
        scratch_shapes=[pltpu.VMEM((rows, d), F32)] + [pltpu.VMEM((rows, d), BF16)] * 5
        + [pltpu.VMEM((block, d), F32), pltpu.SemaphoreType.DMA((5 * rows // block,)), pltpu.SemaphoreType.DMA((rows // block,))],
        out_shape=[jax.ShapeDtypeStruct((rows, d), BF16), jax.ShapeDtypeStruct((1, d), F32)],
        compiler_params=pltpu.CompilerParams(vmem_limit_bytes=VMEM),
        cost_estimate=_cost(rows * d * HEAD),
        name="finish",
    )(dep, own, *sent, x, dy, gain.reshape(1, d))


def _add_up(part, total, all_s, sem, send_sem, recv_sem):
    me = lax.axis_index("tp")
    others = [_block(me, r) for r in range(1, 8)]
    mine = pltpu.make_async_copy(part, all_s.at[me], sem)
    mine.start()
    _greet(others)
    sends = [_remote(part, all_s.at[me], send_sem.at[i], recv_sem.at[me], other) for i, other in enumerate(others)]
    for copy in sends:
        copy.start()
    mine.wait()
    for other in others:
        pltpu.make_async_copy(part, all_s.at[other], recv_sem.at[other]).wait()
    total[...] = sum(all_s[i] for i in range(1, 8)) + all_s[0]
    for copy in sends:
        copy.wait_send()


def add_up(part):
    dma = pltpu.SemaphoreType.DMA
    return pl.pallas_call(
        _add_up, in_specs=[ANY], out_specs=IN_VMEM,
        scratch_shapes=[pltpu.VMEM((8, *part.shape), F32), dma, dma((7,)), dma((8,))],
        out_shape=jax.ShapeDtypeStruct(part.shape, F32),
        compiler_params=_meeting(2),
        name="add_up",
    )(part)


def swap(value, r):
    return lax.ppermute(value, "tp", [(i, i ^ r) for i in range(8)])


def normed(x, gain):
    wide = x.astype(F32)
    scale = lax.rsqrt(jnp.mean(wide * wide, -1, keepdims=True) + 1e-6)
    return (wide * scale * gain.astype(F32)).astype(BF16)


def gather(halves):
    got = {(0, i): t for i, t in enumerate(halves)}

    def send(r, i, by):
        got[r, i] = swap(got[r ^ by, i], by)

    for r, i in ((4, 0), (2, 1), (4, 1), (2, 0)):
        send(r, i, r)
    send(6, 0, 2)
    send(6, 1, 4)
    return got


def solution(mesh):
    def step(x, dy, gain, wq, wk, wv, wo):
        me = lax.axis_index("tp").astype(jnp.int32).reshape(1)
        rows, weights = x.shape[0] * 8, [wq, wk, wv]
        angle = jnp.arange(rows).astype(F32)[:, None] * THETA ** (-jnp.arange(HEAD // 2, dtype=F32) / (HEAD // 2))
        cos, sin = jnp.cos(angle), jnp.sin(angle)
        cos_w, sin_w = jnp.concatenate([cos, cos], 1), jnp.concatenate([-sin, sin], 1)
        cos_t, sin_t = cos.T, sin.T
        both = lambda r: [(r, 0), (r, 1)]
        both = lambda r: [(r, 0), (r, 1)]
        order = [both(0), [(4, 0), (2, 1)], [(4, 1), (2, 0)], both(6)]

        a = gather([normed(x[:HALF], gain), normed(x[HALF:], gain)])

        def projected(n, token, before, through=()):
            return project(token, 3 + n, [a[key] for key in order[n]], order[n], weights, cos_w, sin_w, before, through)

        def seen_grad(n, token, before):
            return by_seen(token, 7 + n, [g[key] for key in order[n]], order[n], wo, rows, before)

        *known, token = projected(0, jnp.zeros(TOKEN.shape, F32), [])
        *known, g0, g1, token = projected(1, token, known, [dy[:HALF], dy[HALF:]])
        g = gather([g0, g1])
        *known, token = projected(2, token, known)
        *grads, token = seen_grad(0, token, [])
        *known, token = projected(3, token, known)
        q, k, v, states = known
        out, lse, token = attend(token, me, q, k, v)
        heads = q.shape[0]

        def attention_back(rs, token, before, last):
            return back(token, me, rs, q, k, v, grads[0].reshape(heads, HEAD, rows), out, lse, cos_t, sin_t, before, last)

        *sums, token = attention_back((0,), token, None, False)
        *grads, token = seen_grad(1, token, grads)
        *grads, token = seen_grad(2, token, grads)
        *sums, token = attention_back((4, 2), token, sums, False)
        *grads, token = seen_grad(3, token, grads)
        dq, dq_t, dkv, dkv_t, token = attention_back((6,), token, sums, True)

        def term(token, keys, groups, adds=(), dtypes=(BF16,) * 4):
            return by_states(token, keys, dq, dkv, weights, adds, groups, dtypes)

        s60, s61, token = exchange(token, both(7), both(6), [], dq, dkv, weights, 0)
        far2, far4 = swap(s60, 4), swap(s61, 2)
        s40, s21, got, t1, token = exchange(token, [(5, 0), (3, 1), (5, 1), (3, 0)], [(4, 0), (2, 1)], both(1), dq, dkv, weights, 1)
        r40, r21 = swap(s40, 4), swap(s21, 2)
        p0 = swap(t1, 1)
        by_o, token = by_wo(token, me, grads[1], out.reshape(heads * HEAD, rows))
        s41, s20, own, token = term(token, [(4, 1), (2, 0)] + both(0), [1, 1, 2],
                                    [(0, got, 0), (0, far4, 0), (1, got, 1), (1, far2, 0), (2, p0, 0), (3, p0, 1)], (BF16, BF16, F32))
        r41, r20 = swap(s41, 4), swap(s20, 2)
        *by_w, token = by_qkv(token, me, states, dq_t, dkv_t, 0, 7, [])
        by_x, by_gain = finish(token, own, [r40, r41, r20, r21], x, dy, gain)
        return (by_x, add_up(by_gain), *by_w, by_o)

    tokens, columns = P(("dp", "tp"), None), P(None, "tp")
    return jax.shard_map(
        step,
        mesh=mesh,
        in_specs=(tokens, tokens, P(None), columns, columns, columns, P("tp", None)),
        out_specs=(tokens, P("dp", None), P("dp", "tp"), P("dp", "tp"), P("dp", "tp"), P(("dp", "tp"), None)),
        check_vma=False,
    )
```

```python
import functools

import jax
import jax.numpy as jnp
from jax import lax
from jax.experimental import pallas as pl
from jax.experimental.pallas import tpu as pltpu
from jax.sharding import PartitionSpec as P


HEAD = 128
THETA = 10000
NEG = -1e30
HIDDEN = 2 * NEG
LOG2E = 1.4426950408889634
VMEM = 67043328
F32, BF16 = jnp.float32, jnp.bfloat16
ANY = pl.BlockSpec(memory_space=pltpu.HBM)
IN_VMEM = pl.BlockSpec(memory_space=pltpu.VMEM)
TOKEN = jax.ShapeDtypeStruct((8, 128), F32)
TOKEN_SPEC = pl.BlockSpec(TOKEN.shape, lambda i, _: (0, 0))


def _dot(a, b, ca, cb):
    return lax.dot_general(a, b, (((ca,), (cb,)), ((), ())), preferred_element_type=F32)


def _params():
    return pltpu.CompilerParams(dimension_semantics=("arbitrary",), vmem_limit_bytes=VMEM)


def _meeting(collective_id):
    return pltpu.CompilerParams(vmem_limit_bytes=VMEM, collective_id=collective_id, has_side_effects=True)


def _sems(n):
    return pltpu.SemaphoreType.DMA((n,))


def _cost(products):
    return pl.CostEstimate(flops=2 * products, bytes_accessed=products // 64, transcendentals=0)


def _whole(*shape):
    return pl.BlockSpec(shape, lambda i, _: (0, 0))


HALF = 128


def _block(me, r):
    bits = [(4, lax.div(me, 4)), (2, lax.rem(lax.div(me, 2), 2)), (1, lax.rem(me, 2))]
    return sum(n * ((1 - bit) if r & n else bit) for n, bit in bits)


def _at(me, key):
    return pl.multiple_of((_block(me, key[0]) * 2 + key[1]) * HALF, HALF)


def _rows(n):
    return [pl.ds(i * HALF, HALF) for i in range(n)]


def _parts(size, cuts=(0, 1, 3, 5, 7)):
    return [pl.ds(lo * size // 7, (hi - lo) * size // 7) for lo, hi in zip(cuts, cuts[1:])]


def _pairs(keys):
    return keys + [(r ^ 1, i) for r, i in keys]


class _Copies:
    def __init__(self, sem):
        self.sem, self.used = sem, 0

    def start(self, pairs):
        made = []
        for src, dst in pairs:
            made.append(pltpu.make_async_copy(src, dst, self.sem.at[self.used]))
            made[-1].start()
            self.used += 1
        return made


class _Stream:
    def __init__(self, copies, parts, pairs):
        self.copies, self.parts, self.pairs, self.made = copies, parts, pairs, []
        self.more()

    def more(self):
        if len(self.made) < len(self.parts):
            self.made.append(self.copies.start(self.pairs(self.parts[len(self.made)])))

    def take(self, c):
        if c == 0:
            self.more()
        _wait(self.made[c])
        self.more()


def _greet(others):
    barrier = pltpu.get_barrier_semaphore()
    for other in others:
        pl.semaphore_signal(barrier, inc=1, device_id={"tp": other}, device_id_type=pl.DeviceIdType.MESH)
    pl.semaphore_wait(barrier, len(others))


def _remote(src, dst, send_sem, recv_sem, other):
    return pltpu.make_async_remote_copy(src_ref=src, dst_ref=dst, send_sem=send_sem, recv_sem=recv_sem, device_id={"tp": other},
                                        device_id_type=pl.DeviceIdType.MESH)


def _crossing(pieces, target, parts, rows, send_sem, recv_sem):
    other, n = _block(lax.axis_index("tp"), 1), len(pieces)
    _greet([other])
    made = [[_remote(p.at[:, part], target.at[r, part], send_sem.at[c * n + i], recv_sem.at[c * n + i], other) for i, (p, r) in enumerate(zip(pieces, rows))]
            for c, part in enumerate(parts)]
    for x in sum(made, []):
        x.start()
    return made


def _wait(copies):
    for c in copies:
        c.wait()


def _stacked(weights, w_s, part):
    at, pairs = 0, []
    for w in weights:
        pairs.append((w.at[part, :], w_s.at[part, at : at + w.shape[1]]))
        at += w.shape[1]
    return pairs


def _project(dep, *refs, keys, heads, extra, through):
    n, me = len(keys), lax.axis_index("tp")
    pieces, (wq, wk, wv, cos, sin), refs = refs[:n], refs[n : n + 5], refs[n + 5 + extra :]
    q_hbm, k_hbm, v_hbm, a_hbm = refs[:4]
    tok, a_s, w_s, cos_s, sin_s, acc, q_s, k_s, v_s, sem, send_sem, recv_sem = refs[4 + through :]
    tok[...] = jnp.zeros_like(tok)
    rows, tokens = _rows(2 * n), [pl.ds(_at(me, key), HALF) for key in _pairs(keys)]
    copies, parts = _Copies(sem), _parts(a_s.shape[1])
    loads = _Stream(copies, parts, lambda part: [(p.at[:, part], a_s.at[r, part]) for p, r in zip(pieces, rows)] + _stacked((wq, wk, wv), w_s, part))
    tables = copies.start([(t.at[there, :], s.at[r, :]) for t, s in ((cos, cos_s), (sin, sin_s)) for r, there in zip(rows, tokens)])
    crossing = _crossing(pieces, a_s, parts, rows[n:], send_sem, recv_sem)
    for c, part in enumerate(parts):
        loads.take(c)
        for x in crossing[c]:
            x.wait_recv()
        if part is parts[-1]:
            stores = copies.start([(a_s.at[r, :], a_hbm.at[there, :]) for r, there in zip(rows, tokens)])
        got = _dot(a_s[:, part], w_s[part, :], 1, 0)
        acc[...] = got if c == 0 else acc[...] + got
    _wait(tables)
    for h in range(heads + 2):
        t = acc[:, h * HEAD : (h + 1) * HEAD].astype(BF16)
        if h <= heads:
            t = t.astype(F32)
            t = (t * cos_s[...] + pltpu.roll(t, HEAD // 2, 1) * sin_s[...]).astype(BF16)
        if h < heads:
            q_s[h] = t
        else:
            (k_s if h == heads else v_s)[...] = t
    for r, there in zip(rows, tokens):
        stores += copies.start([(q_s.at[:, r, :], q_hbm.at[:, there, :]), (k_s.at[r, :], k_hbm.at[there, :]), (v_s.at[r, :], v_hbm.at[there, :])])
    _wait(stores)
    for x in sum(crossing, []):
        x.wait_send()


def project(dep, collective_id, pieces, keys, weights, cos, sin, before, through=()):
    (d, width), more = weights[0].shape, weights[1].shape[1]
    heads, rows, n, full = width // HEAD, cos.shape[0], len(pieces), width + 2 * more
    total, extra = 2 * n * HALF, len(before) + len(through)
    outs = [jax.ShapeDtypeStruct(s, BF16) for s in ((heads, rows, HEAD), (rows, HEAD), (rows, HEAD), (rows, d))]
    outs += [jax.ShapeDtypeStruct(t.shape, t.dtype) for t in through]
    first = 1 + n + 5
    return pl.pallas_call(
        functools.partial(_project, keys=keys, heads=heads, extra=extra, through=len(through)),
        in_specs=[ANY] * (first + extra), out_specs=[ANY] * len(outs) + [IN_VMEM],
        scratch_shapes=[pltpu.VMEM((total, d), BF16), pltpu.VMEM((d, full), BF16), pltpu.VMEM((total, HEAD), F32), pltpu.VMEM((total, HEAD), F32),
                            pltpu.VMEM((total, full), F32), pltpu.VMEM((heads, total, HEAD), BF16), pltpu.VMEM((total, HEAD), BF16),
                            pltpu.VMEM((total, HEAD), BF16), _sems(20 * n + 12), _sems(4 * n), _sems(4 * n)],
        out_shape=outs + [TOKEN],
        input_output_aliases={first + i: len(outs) - extra + i for i in range(extra)},
        compiler_params=_meeting(collective_id),
        cost_estimate=_cost(total * d * full),
        name="project",
    )(dep, *pieces, *weights, cos, sin, *before, *through)


def _by_seen(dep, *refs, keys, extra):
    n, me = len(keys), lax.axis_index("tp")
    pieces, wo, (out_hbm, g_hbm, tok, g_s, w_s, acc, stage, sem, send_sem, recv_sem) = refs[:n], refs[n], refs[n + 1 + extra :]
    tok[...] = jnp.zeros_like(tok)
    rows, tokens = _rows(2 * n), [pl.ds(_at(me, key), HALF) for key in _pairs(keys)]
    copies, parts = _Copies(sem), _parts(g_s.shape[1])
    loads = _Stream(copies, parts, lambda part: [(p.at[:, part], g_s.at[r, part]) for p, r in zip(pieces, rows)] + [(wo.at[:, part], w_s.at[:, part])])
    crossing = _crossing(pieces, g_s, parts, rows[n:], send_sem, recv_sem)
    for c, part in enumerate(parts):
        loads.take(c)
        for x in crossing[c]:
            x.wait_recv()
        if part is parts[-1]:
            stores = copies.start([(g_s.at[r, :], g_hbm.at[there, :]) for r, there in zip(rows, tokens)])
        got = _dot(w_s[:, part], g_s[:, part], 1, 1)
        acc[...] = got if c == 0 else acc[...] + got
    stage[...] = acc[...].astype(BF16)
    _wait(stores + copies.start([(stage.at[:, r], out_hbm.at[:, there]) for r, there in zip(rows, tokens)]))
    for x in sum(crossing, []):
        x.wait_send()


def by_seen(dep, collective_id, pieces, keys, wo, rows, before):
    width, d = wo.shape
    n, extra = len(pieces), len(before)
    total = 2 * n * HALF
    return pl.pallas_call(
        functools.partial(_by_seen, keys=keys, extra=extra),
        in_specs=[ANY] * (n + 2 + extra), out_specs=[ANY, ANY, IN_VMEM],
        scratch_shapes=[pltpu.VMEM((total, d), BF16), pltpu.VMEM((width, d), BF16), pltpu.VMEM((width, total), F32), pltpu.VMEM((width, total), BF16),
                            _sems(12 * n + 4), _sems(4 * n), _sems(4 * n)],
        out_shape=[jax.ShapeDtypeStruct((width, rows), BF16), jax.ShapeDtypeStruct((rows, d), BF16), TOKEN],
        input_output_aliases={2 + n + i: i for i in range(extra)},
        compiler_params=_meeting(collective_id),
        cost_estimate=_cost(total * d * width),
        name="by_seen",
    )(dep, *pieces, wo, *before)


def _attend(me, dep, q_ref, k_ref, v_ref, o_ref, lse_ref, tok, top_s, mix_s, gap_s, *, scale, bq):
    g, d = q_ref.shape[0], q_ref.shape[2]
    iq = pl.program_id(0)
    e = scale * LOG2E

    @pl.when(iq == 0)
    def _():
        tok[...] = jnp.zeros_like(tok)
        gap_s[...] = lax.broadcasted_iota(jnp.int32, gap_s.shape, 1) - lax.broadcasted_iota(jnp.int32, gap_s.shape, 0)

    top_s[...] = jnp.full_like(top_s, NEG)
    mix_s[...] = jnp.zeros_like(mix_s)

    def block(first, keys, lo, masked):
        here, there = pl.ds(pl.multiple_of(first, keys), keys), pl.ds(lo, bq - lo)
        scores = [_dot(k_ref[here, :], q_ref[n, there, :], 1, 1) for n in range(g)]
        weights, keeps = [], []
        for n, s in enumerate(scores):
            if masked:
                s = jnp.where(gap_s[:keys, : bq - lo] >= 0, s, HIDDEN)
            old = top_s[n : n + 1, there]
            top = jnp.maximum(old, s.max(axis=0, keepdims=True))
            top_s[n : n + 1, there] = top
            weights.append(jnp.exp2((s - top) * e).astype(BF16))
            keeps.append(jnp.exp2((old - top) * e))
        values = jnp.concatenate([v_ref[here, :].T, jnp.ones((8, keys), BF16)], axis=0)
        for n, (p, keep) in enumerate(zip(weights, keeps)):
            mix_s[n, :, there] = mix_s[n, :, there] * keep + _dot(values, p, 1, 0)

    lax.fori_loop(0, iq, lambda j, _: block(j * bq, bq, 0, False), None)
    for lo in (0, bq // 2):
        block(iq * bq + lo, bq // 2, lo, True)
    for n in range(g):
        total = mix_s[n, d : d + 1, :]
        o_ref[n] = (mix_s[n, :d, :] * (1 / total)).astype(BF16)
        lse_ref[n : n + 1, :] = top_s[n : n + 1, :] * scale + jnp.log(total)


def attend(dep, me, q, k, v, bq=512):
    g, rows, d = q.shape
    whole = _whole(rows, d)
    return pl.pallas_call(
        functools.partial(_attend, scale=d**-0.5, bq=bq),
        grid_spec=pltpu.PrefetchScalarGridSpec(
            num_scalar_prefetch=1, grid=(rows // bq,),
            in_specs=[ANY, pl.BlockSpec((g, bq, d), lambda i, _: (0, i, 0)), whole, whole],
            out_specs=[pl.BlockSpec((g, d, bq), lambda i, _: (0, 0, i)), pl.BlockSpec((g, bq), lambda i, _: (0, i)),
                       TOKEN_SPEC],
            scratch_shapes=[pltpu.VMEM((g, bq), F32), pltpu.VMEM((g, d + 8, bq), F32), pltpu.VMEM((bq // 2, bq), jnp.int32)]),
        out_shape=[jax.ShapeDtypeStruct((g, d, rows), BF16), jax.ShapeDtypeStruct((g, rows), F32), TOKEN],
        compiler_params=_params(),
        cost_estimate=_cost(2 * g * rows * rows * d),
        name="attend",
    )(me, dep, q, k, v)


def _chip(me, i, rs):
    r = rs[0]
    for n in range(1, len(rs)):
        r = jnp.where(i == n, rs[n], r)
    return (me[0] ^ r) // 2


def _back(me, dep, q_ref, k_ref, v_ref, do_ref, o_ref, lse_ref, cos, sin, *refs, scale, bq, first, last, rs):
    g, d = q_ref.shape[0], q_ref.shape[2]
    if not first:
        dk_in, dv_in, refs = refs[0], refs[1], refs[2 + (2):]
    if last:
        dq_ref, dqt_ref, dkv_ref, dkvt_ref, tok, dq_s, gap_s, dk_s, dv_s = refs
    else:
        dq_ref, dqt_ref, dk_s, dv_s, tok, dq_s, gap_s = refs
    i = pl.program_id(0)
    iq = _chip(me, i, rs)
    e = scale * LOG2E
    half = d // 2

    @pl.when(i == 0)
    def _():
        tok[...] = jnp.zeros_like(tok)
        gap_s[...] = lax.broadcasted_iota(jnp.int32, gap_s.shape, 1) - lax.broadcasted_iota(jnp.int32, gap_s.shape, 0)
        if first:
            dk_s[...] = jnp.zeros_like(dk_s)
            dv_s[...] = jnp.zeros_like(dv_s)
        else:
            dk_s[...] = dk_in[...]
            dv_s[...] = dv_in[...]

    dq_s[...] = jnp.zeros_like(dq_s)
    lses = [lse_ref[n : n + 1, :] * LOG2E for n in range(g)]
    deltas = [(do_ref[n].astype(F32) * o_ref[n].astype(F32)).sum(0, keepdims=True) for n in range(g)]

    def block(first, keys, lo, masked):
        here, there = pl.ds(pl.multiple_of(first, keys), keys), pl.ds(lo, bq - lo)
        scores = [_dot(k_ref[here, :], q_ref[n, there, :], 1, 1) for n in range(g)]
        dps = [_dot(v_ref[here, :], do_ref[n, :, there], 1, 0) for n in range(g)]
        kt = k_ref[here, :].T
        for n in range(g):
            p = jnp.exp2(scores[n] * e - lses[n][:, lo:])
            if masked:
                p = jnp.where(gap_s[:keys, : bq - lo] >= 0, p, 0.0)
            ds = (p * (dps[n] - deltas[n][:, lo:])).astype(BF16)
            dv_s[here, :] += _dot(p.astype(BF16), do_ref[n, :, there], 1, 1)
            dk_s[here, :] += _dot(ds, q_ref[n, there, :], 1, 0)
            dq_s[n, :, there] += _dot(kt, ds, 1, 0)

    lax.fori_loop(0, iq, lambda j, _: block(j * bq, bq, 0, False), None)
    for lo in (0, bq // 2):
        block(iq * bq + lo, bq // 2, lo, True)

    def unturned(t, c, s):
        t = t.astype(BF16).astype(F32)
        a, b = t[:half], t[half:]
        return jnp.concatenate([a * c + b * s, b * c - a * s], axis=0)

    at = pl.ds(pl.multiple_of(iq * bq, bq), bq)
    for n in range(g):
        t = unturned(dq_s[n] * scale, cos[:, at], sin[:, at])
        dqt_ref[n * d : (n + 1) * d, :] = t.astype(BF16)
        dq_ref[:, n * d : (n + 1) * d] = t.T.astype(BF16)

    if last:
        @pl.when(i == len(rs) - 1)
        def _():
            t = unturned((dk_s[...] * scale).T, cos[...], sin[...])
            dkvt_ref[:d, :] = t.astype(BF16)
            dkv_ref[:, :d] = t.T.astype(BF16)
            dkvt_ref[d:, :] = dv_s[...].T.astype(BF16)
            dkv_ref[:, d:] = dv_s[...].astype(BF16)


def back(dep, me, rs, q, k, v, do_t, out_t, lse, cos_t, sin_t, before, last):
    g, rows, d = q.shape
    first, bq = before is None, rows // 4
    here = lambda i, me: _chip(me, i, rs)
    whole = _whole(rows, d)
    table = _whole(d // 2, rows)
    across = pl.BlockSpec((g, d, bq), lambda i, me: (0, 0, here(i, me)))
    specs = [ANY, pl.BlockSpec((g, bq, d), lambda i, me: (0, here(i, me), 0)), whole, whole, across, across, pl.BlockSpec((g, bq), lambda i, me: (0, here(i, me))), table, table]
    given = [dep, q, k, v, do_t, out_t, lse, cos_t, sin_t]
    aliases = {}
    if not first:
        specs += [whole, whole, ANY, ANY]
        given += [before[2], before[3], before[0], before[1]]
        aliases = {2 + 10: 0, 2 + 11: 1}
    outs = [jax.ShapeDtypeStruct((rows, g * d), BF16), jax.ShapeDtypeStruct((g * d, rows), BF16)]
    out_specs = [pl.BlockSpec((bq, g * d), lambda i, me: (here(i, me), 0)), pl.BlockSpec((g * d, bq), lambda i, me: (0, here(i, me)))]
    scratch = [pltpu.VMEM((g, d, bq), F32), pltpu.VMEM((bq // 2, bq), jnp.int32)]
    if last:
        outs += [jax.ShapeDtypeStruct((rows, 2 * d), BF16), jax.ShapeDtypeStruct((2 * d, rows), BF16)]
        out_specs += [_whole(rows, 2 * d), _whole(2 * d, rows)]
        scratch += [pltpu.VMEM((rows, d), F32)] * 2
    else:
        outs += [jax.ShapeDtypeStruct((rows, d), F32)] * 2
        out_specs += [whole, whole]
    return pl.pallas_call(
        functools.partial(_back, scale=d**-0.5, bq=bq, first=first, last=last, rs=rs),
        grid_spec=pltpu.PrefetchScalarGridSpec(num_scalar_prefetch=1, grid=(len(rs),), in_specs=specs,
                                               out_specs=out_specs + [pl.BlockSpec((8, 128), lambda i, b: (0, 0))], scratch_shapes=scratch),
        out_shape=outs + [TOKEN],
        input_output_aliases=aliases,
        compiler_params=_params(),
        cost_estimate=_cost(4 * g * len(rs) * bq * rows * d),
        name="back",
    )(me, *given)


def _by_states(dep, dq, dkv, wq, wk, wv, *refs, keys, adds, groups):
    n, many, me = len(keys), len(groups), lax.axis_index("tp")
    added, outs, tok, refs = refs[: len(adds)], refs[len(adds) : len(adds) + many], refs[len(adds) + many], refs[len(adds) + many + 1 :]
    stages, (lhs_s, w_s, add_s, sem) = refs[:many], refs[many:]
    tok[...] = jnp.zeros_like(tok)
    rows, cols = _rows(n + len(adds)), dq.shape[1]
    copies, parts = _Copies(sem), _parts(w_s.shape[0])
    first = []
    for key, r in zip(keys, rows):
        there = pl.ds(_at(me, key), HALF)
        first += copies.start([(dq.at[there, :], lhs_s.at[r, :cols]), (dkv.at[there, :], lhs_s.at[r, cols:])])
    loads = _Stream(copies, parts, lambda part: _stacked((wq, wk, wv), w_s, part)
                    + [(a.at[_rows(row + 1)[row], part], add_s.at[r, part]) for a, (_, row), r in zip(added, adds, rows)])
    _wait(first)
    place, stores = [(o, r) for o, k in enumerate(groups) for r in _rows(k)], []
    for c, part in enumerate(parts):
        loads.take(c)
        got = _dot(lhs_s[...], w_s[part, :], 1, 1)
        for i, (o, r) in enumerate(place):
            t = got[i * HALF : (i + 1) * HALF]
            for (target, _), mine in zip(adds, rows):
                if target == i:
                    t = t + add_s[mine, part].astype(F32)
            stages[o][r, part] = t.astype(stages[o].dtype)
        stores += copies.start([(stage.at[:, part], out.at[:, part]) for stage, out in zip(stages, outs)])
    _wait(stores)


def by_states(dep, keys, dq, dkv, weights, adds, groups, dtypes):
    d, n, many, full = weights[0].shape[0], len(keys), len(adds), sum(w.shape[1] for w in weights)
    shapes = [((k * HALF, d), t) for k, t in zip(groups, dtypes)]
    return pl.pallas_call(
        functools.partial(_by_states, keys=keys, adds=[(i, row) for i, _, row in adds], groups=groups),
        in_specs=[ANY] * (6 + many), out_specs=[ANY] * len(groups) + [IN_VMEM],
        scratch_shapes=[pltpu.VMEM(*s) for s in shapes] + [pltpu.VMEM((n * HALF, full), BF16), pltpu.VMEM((d, full), BF16),
                                                               pltpu.VMEM((max(many, 1) * HALF, d), BF16),
                                                               _sems(2 * n + 4 * (3 + many + len(groups)))],
        out_shape=[jax.ShapeDtypeStruct(*s) for s in shapes] + [TOKEN],
        compiler_params=pltpu.CompilerParams(vmem_limit_bytes=VMEM),
        cost_estimate=_cost(n * HALF * d * full),
        name="by_states",
    )(dep, dq, dkv, *weights, *(a for _, a, _ in adds))


def _exchange(dep, dq, dkv, wq, wk, wv, *refs, give, keep, plain):
    n, late, some = len(keep), len(give) > len(keep), len(plain) > 0
    kept, late_hbm, plain_hbm, tok = refs[:n], refs[n], refs[n + some], refs[n + late + some]
    lhs_s, w_s, give_s, got_s, sum_s, out_s, sem, send_sem, recv_sem = refs[n + late + some + 1 :]
    tok[...] = jnp.zeros_like(tok)
    me = lax.axis_index("tp")
    other = _block(me, 1)
    d, cols, mine = w_s.shape[0], dq.shape[1], n * HALF
    copies, parts, rows = _Copies(sem), _parts(d, (0, 1, 3, 5, 6, 7)), _rows(len(give) + len(plain) + n)
    given, out = len(give) * HALF, (len(give) + len(plain)) * HALF
    first = []
    for key, row in zip(give + plain + keep, rows):
        there = pl.ds(_at(me, key), HALF)
        first += copies.start([(dq.at[there, :], lhs_s.at[row, :cols]), (dkv.at[there, :], lhs_s.at[row, cols:])])
    loads = _Stream(copies, parts, lambda part: _stacked((wq, wk, wv), w_s, part))
    _greet([other])
    _wait(first)

    def crossing(c):
        pairs = [(give_s.at[:mine, parts[c]], got_s.at[:, parts[c]])]
        if late:
            pairs.append((give_s.at[mine:given, parts[c]], late_hbm.at[:, parts[c]]))
        at = [c * len(pairs) + i for i in range(len(pairs))]
        return [_remote(a, b, send_sem.at[m], recv_sem.at[m], other) for m, (a, b) in zip(at, pairs)]

    def add(c):
        for x in sent[c]:
            x.wait_recv()
        wide = parts[c].size
        out_s[:, parts[c]] = (sum_s[c % 2, :, :wide] + got_s[:, parts[c]].astype(F32)).astype(BF16)
        return copies.start([(out_s.at[rows[i], parts[c]], kept[i].at[:, parts[c]]) for i in range(n)])

    sent, stores = [], []
    for c, part in enumerate(parts):
        loads.take(c)
        for lo in range(0, part.size, 512):
            some_columns = pl.ds(part.start + lo, 512)
            got = _dot(lhs_s[...], w_s[some_columns, :], 1, 1)
            give_s[:, some_columns] = got[:out].astype(BF16)
            sum_s[c % 2, :, lo : lo + 512] = got[out:]
        if c:
            stores += add(c - 1)
        sent.append(crossing(c))
        for x in sent[c]:
            x.start()
        if some:
            stores += copies.start([(give_s.at[given:, part], plain_hbm.at[:, part])])
    stores += add(len(parts) - 1)
    _wait(stores)
    for x in sum(sent, []):
        x.wait_send()


def exchange(dep, give, keep, plain, dq, dkv, weights, collective_id):
    d, n, full = weights[0].shape[0], len(keep), sum(w.shape[1] for w in weights)
    more, parts = len(give) - n, 5
    outs = [jax.ShapeDtypeStruct((HALF, d), BF16)] * n + [jax.ShapeDtypeStruct((m * HALF, d), BF16) for m in (more, len(plain)) if m]
    total = len(give) + len(plain) + n
    return pl.pallas_call(
        functools.partial(_exchange, give=give, keep=keep, plain=plain),
        in_specs=[ANY] * 6, out_specs=[ANY] * len(outs) + [IN_VMEM],
        scratch_shapes=[pltpu.VMEM((total * HALF, full), BF16), pltpu.VMEM((d, full), BF16), pltpu.VMEM(((total - n) * HALF, d), BF16),
                        pltpu.VMEM((n * HALF, d), BF16), pltpu.VMEM((2, n * HALF, 2 * d // 7), F32), pltpu.VMEM((n * HALF, d), BF16),
                        pltpu.SemaphoreType.DMA((2 * total + parts * (4 + n),)), pltpu.SemaphoreType.DMA((2 * parts,)), pltpu.SemaphoreType.DMA((2 * parts,))],
        out_shape=outs + [TOKEN],
        compiler_params=_meeting(collective_id),
        cost_estimate=_cost(total * HALF * d * full),
        name="exchange",
    )(dep, dq, dkv, *weights)


def _by_qkv(me, dep, a, dqt, dkvt, *refs, extra):
    gq, gk, gv, tok, r_s = refs[extra:]
    tok[...] = jnp.zeros_like(tok)
    wide = dqt.shape[0]
    r_s[:wide] = _dot(dqt[...], a[...], 1, 0)
    r_s[wide:] = _dot(dkvt[...], a[...], 1, 0)
    for h in range(r_s.shape[0] // HEAD):
        t = r_s[h * HEAD : (h + 1) * HEAD].T.astype(BF16)
        if h * HEAD < wide:
            gq[:, h * HEAD : (h + 1) * HEAD] = t
        else:
            (gk if h * HEAD == wide else gv)[...] = t


def by_qkv(dep, me, a, dqt, dkvt, lo, hi, before, bm=1024):
    (rows, d), width, extra = a.shape, dqt.shape[0], len(before)
    return pl.pallas_call(
        functools.partial(_by_qkv, extra=extra),
        grid_spec=pltpu.PrefetchScalarGridSpec(
            num_scalar_prefetch=1, grid=(hi - lo,),
            in_specs=[ANY, pl.BlockSpec((rows, bm), lambda j, _: (0, lo + j)), _whole(*dqt.shape), _whole(*dkvt.shape)] + [ANY] * extra,
            out_specs=[pl.BlockSpec((bm, w), lambda j, _: (lo + j, 0)) for w in (width, HEAD, HEAD)] + [TOKEN_SPEC],
            scratch_shapes=[pltpu.VMEM((width + 2 * HEAD, bm), F32)]),
        out_shape=[jax.ShapeDtypeStruct((d, w), BF16) for w in (width, HEAD, HEAD)] + [TOKEN],
        input_output_aliases={5 + i: i for i in range(extra)},
        compiler_params=_params(),
        cost_estimate=_cost(rows * (hi - lo) * bm * (width + 2 * HEAD)),
        name="by_qkv",
    )(me, dep, a, dqt, dkvt, *before)


def _by_wo(me, dep, g, seen_t, out, tok):
    tok[...] = jnp.zeros_like(tok)
    out[...] = _dot(seen_t[...], g[...], 1, 0).astype(BF16)


def by_wo(dep, me, g, seen_t, bn=1024):
    (rows, d), width = g.shape, seen_t.shape[0]
    return pl.pallas_call(
        _by_wo,
        grid_spec=pltpu.PrefetchScalarGridSpec(
            num_scalar_prefetch=1, grid=(d // bn,), in_specs=[ANY, pl.BlockSpec((rows, bn), lambda j, _: (0, j)), _whole(width, rows)],
            out_specs=[pl.BlockSpec((width, bn), lambda j, _: (0, j)), TOKEN_SPEC]),
        out_shape=[jax.ShapeDtypeStruct((width, d), BF16), TOKEN],
        compiler_params=_params(),
        cost_estimate=_cost(rows * d * width),
        name="by_wo",
    )(me, dep, g, seen_t)


def _finish(dep, own, r40, r41, r20, r21, x, dy, gain, by_x, by_gain, own_s, far_s, near_s, x_s, dy_s, out_s, sum_s, sem, out_sem, *, block, wide):
    _, d = own_s.shape
    steps, columns = HALF // block, [pl.ds(c, wide) for c in range(0, d, wide)]

    def copies(half, c):
        mine, here = pl.ds(c * block, block), pl.ds(half * HALF + c * block, block)
        pairs = [(x.at[here, :], x_s), (own.at[here, :], own_s), ((r40, r41)[half].at[mine, :], far_s), ((r20, r21)[half].at[mine, :], near_s), (dy.at[here, :], dy_s)]
        at = (half * steps + c) * len(pairs)
        return here, [pltpu.make_async_copy(a, b.at[here, :], sem.at[at + i]) for i, (a, b) in enumerate(pairs)]

    def result(half, c):
        here = pl.ds(half * HALF + c * block, block)
        return pltpu.make_async_copy(out_s.at[here, :], by_x.at[here, :], out_sem.at[half * steps + c])

    for half in (0, 1):
        for c in range(steps):
            for copy in copies(half, c)[1]:
                copy.start()
    sum_s[...] = jnp.zeros_like(sum_s)
    for half in (0, 1):
        def chunk(c, _):
            here, landed = copies(half, c)
            _wait(landed)
            total = jnp.zeros((block, wide), F32)
            for col in columns:
                total += x_s[here, col].astype(F32) ** 2
            scale = lax.rsqrt(jnp.sum(total, -1, keepdims=True) / d + 1e-6)
            total = jnp.zeros((block, wide), F32)
            for col in columns:
                da = own_s[here, col] + far_s[here, col].astype(F32) + near_s[here, col].astype(F32)
                own_s[here, col] = da
                both = da * (x_s[here, col].astype(F32) * scale)
                sum_s[:, col] += both
                total += both * gain[:, col].astype(F32)
            mean = jnp.sum(total, -1, keepdims=True) / d * scale
            for col in columns:
                inner = own_s[here, col] * gain[:, col].astype(F32) - x_s[here, col].astype(F32) * mean
                out_s[here, col] = (dy_s[here, col].astype(F32) + scale * inner).astype(BF16)
            result(half, c).start()

        lax.fori_loop(0, steps, chunk, None)
    by_gain[...] = jnp.sum(sum_s[...], 0, keepdims=True)
    for half in (0, 1):
        for c in range(steps):
            result(half, c).wait()


def finish(dep, own, sent, x, dy, gain, block=32):
    rows, d = x.shape
    return pl.pallas_call(
        functools.partial(_finish, block=block, wide=d // 7),
        in_specs=[ANY] * 8 + [IN_VMEM], out_specs=[ANY, IN_VMEM],
        scratch_shapes=[pltpu.VMEM((rows, d), F32)] + [pltpu.VMEM((rows, d), BF16)] * 5
        + [pltpu.VMEM((block, d), F32), pltpu.SemaphoreType.DMA((5 * rows // block,)), pltpu.SemaphoreType.DMA((rows // block,))],
        out_shape=[jax.ShapeDtypeStruct((rows, d), BF16), jax.ShapeDtypeStruct((1, d), F32)],
        compiler_params=pltpu.CompilerParams(vmem_limit_bytes=VMEM),
        cost_estimate=_cost(rows * d * HEAD),
        name="finish",
    )(dep, own, *sent, x, dy, gain)


def _add_up(part, total, all_s, sem, send_sem, recv_sem):
    me = lax.axis_index("tp")
    others = [_block(me, r) for r in range(1, 8)]
    mine = pltpu.make_async_copy(part, all_s.at[me], sem)
    mine.start()
    _greet(others)
    mine.wait()
    sends = [_remote(all_s.at[me], all_s.at[me], send_sem.at[i], recv_sem.at[me], other) for i, other in enumerate(others)]
    for copy in sends:
        copy.start()
    for other in others:
        pltpu.make_async_copy(part, all_s.at[other], recv_sem.at[other]).wait()
    total[...] = sum(all_s[i] for i in range(1, 8)) + all_s[0]
    for copy in sends:
        copy.wait_send()


def add_up(part):
    dma = pltpu.SemaphoreType.DMA
    return pl.pallas_call(
        _add_up, in_specs=[ANY], out_specs=IN_VMEM,
        scratch_shapes=[pltpu.VMEM((8, *part.shape), F32), dma, dma((7,)), dma((8,))],
        out_shape=jax.ShapeDtypeStruct(part.shape, F32),
        compiler_params=_meeting(2),
        name="add_up",
    )(part)


def swap(value, r):
    return lax.ppermute(value, "tp", [(i, i ^ r) for i in range(8)])


def normed(x, gain):
    wide = x.astype(F32)
    scale = lax.rsqrt(jnp.mean(wide * wide, -1, keepdims=True) + 1e-6)
    return (wide * scale * gain.astype(F32)).astype(BF16)


def gather(halves):
    got = {(0, i): t for i, t in enumerate(halves)}

    def send(r, i, by):
        got[r, i] = swap(got[r ^ by, i], by)

    for r, i in ((4, 0), (2, 1), (4, 1), (2, 0)):
        send(r, i, r)
    send(6, 0, 2)
    send(6, 1, 4)
    return got


def solution(mesh):
    def step(x, dy, gain, wq, wk, wv, wo):
        me = lax.axis_index("tp").astype(jnp.int32).reshape(1)
        rows, weights = x.shape[0] * 8, [wq, wk, wv]
        angle = jnp.arange(rows).astype(F32)[:, None] * THETA ** (-jnp.arange(HEAD // 2, dtype=F32) / (HEAD // 2))
        cos, sin = jnp.cos(angle), jnp.sin(angle)
        cos_w, sin_w = jnp.concatenate([cos, cos], 1), jnp.concatenate([-sin, sin], 1)
        cos_t, sin_t = cos.T, sin.T
        both = lambda r: [(r, 0), (r, 1)]
        both = lambda r: [(r, 0), (r, 1)]
        order = [both(0), [(4, 0), (2, 1)], [(4, 1), (2, 0)], both(6)]

        a = gather([normed(x[:HALF], gain), normed(x[HALF:], gain)])

        def projected(n, token, before, through=()):
            return project(token, 3 + n, [a[key] for key in order[n]], order[n], weights, cos_w, sin_w, before, through)

        def seen_grad(n, token, before):
            return by_seen(token, 7 + n, [g[key] for key in order[n]], order[n], wo, rows, before)

        *known, token = projected(0, jnp.zeros(TOKEN.shape, F32), [])
        *known, g0, g1, row, token = projected(1, token, known, [dy[:HALF], dy[HALF:], gain.reshape(1, -1)])
        g = gather([g0, g1])
        *known, token = projected(2, token, known)
        *grads, token = seen_grad(0, token, [])
        *known, token = projected(3, token, known)
        q, k, v, states = known
        out, lse, token = attend(token, me, q, k, v)
        heads = q.shape[0]

        def attention_back(rs, token, before, last):
            return back(token, me, rs, q, k, v, grads[0].reshape(heads, HEAD, rows), out, lse, cos_t, sin_t, before, last)

        *sums, token = attention_back((0,), token, None, False)
        *grads, token = seen_grad(1, token, grads)
        *grads, token = seen_grad(2, token, grads)
        *sums, token = attention_back((4, 2), token, sums, False)
        *grads, token = seen_grad(3, token, grads)
        dq, dq_t, dkv, dkv_t, token = attention_back((6,), token, sums, True)

        def term(token, keys, groups, adds=(), dtypes=(BF16,) * 4):
            return by_states(token, keys, dq, dkv, weights, adds, groups, dtypes)

        s60, s61, token = exchange(token, both(7), both(6), [], dq, dkv, weights, 0)
        far2, far4 = swap(s60, 4), swap(s61, 2)
        s40, s21, got, t1, token = exchange(token, [(5, 0), (3, 1), (5, 1), (3, 0)], [(4, 0), (2, 1)], both(1), dq, dkv, weights, 1)
        r40, r21 = swap(s40, 4), swap(s21, 2)
        p0 = swap(t1, 1)
        by_o, token = by_wo(token, me, grads[1], out.reshape(heads * HEAD, rows))
        s41, s20, own, token = term(token, [(4, 1), (2, 0)] + both(0), [1, 1, 2],
                                    [(0, got, 0), (0, far4, 0), (1, got, 1), (1, far2, 0), (2, p0, 0), (3, p0, 1)], (BF16, BF16, F32))
        r41, r20 = swap(s41, 4), swap(s20, 2)
        *by_w, token = by_qkv(token, me, states, dq_t, dkv_t, 0, 7, [])
        by_x, by_gain = finish(token, own, [r40, r41, r20, r21], x, dy, row)
        return (by_x, add_up(by_gain), *by_w, by_o)

    tokens, columns = P(("dp", "tp"), None), P(None, "tp")
    return jax.shard_map(
        step,
        mesh=mesh,
        in_specs=(tokens, tokens, P(None), columns, columns, columns, P("tp", None)),
        out_specs=(tokens, P("dp", None), P("dp", "tp"), P("dp", "tp"), P("dp", "tp"), P(("dp", "tp"), None)),
        check_vma=False,
    )
```
